32 devices in a mesh: row: 4 (over y, x), col: 8 (over z, core).
Axes of the slice: x: 2, y: 2, z: 4, core: 2. Of those that a mesh axis runs over, the one named last changes fastest.
Arguments:
- covariance: float32 [16384, 16384], P('row', 'col'), may hold values from -1 to 560
- seed_index: int32 [128], replicated, may hold values from 0 to 16383, as said below
Outputs:
- basis: float32 [16384, 384], P('row')
- projection: float32 [384, 256], replicated
- first_pass: float32 [384, 256], replicated
The draws below stay inside these ranges and needn't reach their ends.
Inputs may be any that keep to these rules, and one draw needn't show every extreme that they name: `seed_index`: 128 distinct column indices.
All inputs are finite; a program needn't handle non-finite values.
Results may differ from the reference program's by a relative error of at most 0.00019.
Values sent between devices are 32-bit elements; how exact they have to be, the bound alone decides.
A program may use at most 128 MiB of HBM per device.

```python
import jax
import jax.numpy as jnp
from jax import lax

N = 16384
B = 128
ITERS = 2


def draw_covariance(key, part):
    first_key = jax.random.fold_in(key, 11)
    second_key = jax.random.fold_in(key, 12)
    place = jnp.arange(N, dtype=jnp.float32) / jnp.float32(N - 1)
    noise = jax.random.normal(first_key, (N, N), jnp.float32)
    loading = jnp.exp(jax.random.uniform(second_key, (N,), jnp.float32, jnp.log(8.0), jnp.log(40.0)))
    loading = loading * (1.0 + 2.0 * place)
    symmetric = (noise + noise.T) * (3.0 / (2.0 * N) ** 0.5)
    return symmetric + jnp.diag(loading)


def draw_seed_index(key, part):
    order = jax.random.permutation(jax.random.fold_in(key, 21), N)
    return order[:B].astype(jnp.int32)


def setup_inputs(seed: int = 0) -> dict:
    arg_keys = jax.random.split(jax.random.key(seed), 3)
    covariance = draw_covariance(jax.random.fold_in(arg_keys[2], 71), 0)
    seed_index = draw_seed_index(jax.random.fold_in(arg_keys[2], 71), 0)
    return dict(covariance=covariance, seed_index=seed_index)


def product(left, right):
    return jnp.dot(left.astype(jnp.float32), right.astype(jnp.float32), precision=lax.Precision.HIGHEST, preferred_element_type=jnp.float32)

def orthonormal(block):
    gram = product(block.T, block)
    lower = jnp.linalg.cholesky(gram)
    basis_block = jax.scipy.linalg.solve_triangular(lower, block.T, lower=True).T
    return (basis_block, lower.T)

def reference(covariance, seed_index):
    start = jnp.take(covariance, seed_index.astype(jnp.int32), axis=1)
    current, upper = orthonormal(start)
    blocks = [current]
    projection = jnp.zeros(((ITERS + 1) * B, ITERS * B), jnp.float32)
    first_pass = jnp.zeros(((ITERS + 1) * B, ITERS * B), jnp.float32)
    for section in range(ITERS):
        image = product(covariance, current)
        stacked = jnp.concatenate(blocks, axis=1)
        first = product(stacked.T, image)
        once = image - product(stacked, first)
        second = product(stacked.T, once)
        twice = once - product(stacked, second)
        current, upper = orthonormal(twice)
        projection = projection.at[:(section + 1) * B, section * B:(section + 1) * B].set(first + second)
        projection = projection.at[(section + 1) * B:(section + 2) * B, section * B:(section + 1) * B].set(upper)
        first_pass = first_pass.at[:(section + 1) * B, section * B:(section + 1) * B].set(first)
        blocks.append(current)
    basis = jnp.concatenate(blocks, axis=1) * jnp.float32(N ** 0.5)
    return (basis, projection, first_pass)
```

```python
import functools

import jax
import jax.numpy as jnp
from jax import lax
from jax.experimental import pallas as pl
from jax.experimental.pallas import tpu as pltpu
from jax.sharding import PartitionSpec as P

MESH = pl.DeviceIdType.MESH
F32, BF16 = jnp.float32, jnp.bfloat16
ITERS = 2
LIMIT = 66 * 1024 * 1024 - 2 * 1024 * 1024

NN = (((1,), (0,)), ((), ()))
NT = (((1,), (1,)), ((), ()))
TN = (((0,), (0,)), ((), ()))


def dot(left, right, dims):
    return lax.dot_general(left, right, dims, precision=lax.Precision.HIGHEST, preferred_element_type=F32)


def halves(value):
    high = value.astype(BF16)
    return high, (value - high.astype(F32)).astype(BF16)


def dot3(left, right, dims):
    lh, ll = halves(left)
    rh, rl = halves(right)
    go = functools.partial(lax.dot_general, dimension_numbers=dims, preferred_element_type=F32)
    return go(lh, rh) + (go(lh, rl) + go(ll, rh))


def gather_kernel(rows, index_ref, inside_ref, cov_ref, out_ref, buf, sem):
    width, cols = buf.shape
    wide = cols // rows

    def fetch(i, carry):
        pltpu.make_async_copy(cov_ref.at[pl.ds(index_ref[i], 1), :], buf.at[pl.ds(i, 1), :], sem).start()
        return carry

    lax.fori_loop(0, width, fetch, 0, unroll=8)
    pltpu.make_async_copy(cov_ref.at[pl.ds(0, width), :], buf, sem).wait()
    keep = inside_ref[...] > 0
    for n in range(rows):
        out_ref[n] = jnp.where(keep, buf[:, n * wide : (n + 1) * wide], 0.0)


def gather(rows, covariance, seed_index):
    row_count, cols = covariance.shape
    width = seed_index.shape[0]
    offsets = seed_index - lax.axis_index("row") * row_count
    inside = (offsets >= 0) & (offsets < row_count)
    return pl.pallas_call(
        functools.partial(gather_kernel, rows),
        out_shape=jax.ShapeDtypeStruct((rows, width, cols // rows), F32),
        in_specs=[
            pl.BlockSpec(memory_space=pltpu.SMEM),
            pl.BlockSpec(memory_space=pltpu.VMEM),
            pl.BlockSpec(memory_space=pl.ANY),
        ],
        out_specs=pl.BlockSpec(memory_space=pltpu.VMEM),
        scratch_shapes=[pltpu.VMEM((width, cols), F32), pltpu.SemaphoreType.DMA],
        compiler_params=pltpu.CompilerParams(vmem_limit_bytes=8 * 1024 * 1024),
        name="gather",
    )(jnp.clip(offsets, 0, row_count - 1), inside.astype(jnp.int32)[:, None], covariance)


def factor(gram, work):
    width = gram.shape[0]
    down = lax.broadcasted_iota(jnp.int32, (width, width), 0)
    across = lax.broadcasted_iota(jnp.int32, (width, width), 1)
    work[:, :width] = gram
    work[:, width:] = jnp.where(down == across, 1.0, 0.0)
    lane = lax.broadcasted_iota(jnp.int32, (1, width), 1)
    tall = lax.broadcasted_iota(jnp.int32, (width, 1), 0)

    def step(j, carry):
        row = work[pl.ds(j, 1), :]
        pivot = jnp.sum(jnp.where(lane == j, row[:, :width], 0.0), axis=1, keepdims=True)
        now = work[...]
        column = jnp.sum(jnp.where(across == j, now[:, :width], 0.0), axis=1, keepdims=True)
        scale = lax.rsqrt(pivot)
        scale = scale * (1.5 - 0.5 * pivot * scale * scale)
        unit = row * scale
        ratio = jnp.where(tall > j, column * scale, 0.0)
        work[...] = jnp.where(tall == j, unit, now - ratio * unit)
        return carry

    lax.fori_loop(0, width, step, 0)
    upper = jnp.where(down <= across, work[:, :width], 0.0)
    return upper, work[:, width:]


def main_kernel(
    rows, cols, x_ref, cov_ref,
    wide_ref, small_ref,
    ahi, alo, stage, stage_sem, part, rsbuf, rs_send, rs_recv,
    zbuf, up_send, up_recv, dn_send, dn_recv, rowbuf, pl_send, pl_recv, dd_send, dd_recv, own_sem, out_sem,
    a_loc, a_in, a_z, a_full, a_s1, a_r1, a_s2, a_r2, a_s3, a_r3, work,
):
    zs = cols // 2
    width, wide = x_ref.shape[1], x_ref.shape[2]
    row = lax.axis_index("row")
    col = lax.axis_index("col")
    z = col // 2
    core = col % 2
    plane = 2 * rows
    q = row * 2 + core

    barrier = pltpu.get_barrier_semaphore()
    for d in range(1, plane):
        t = lax.rem(q + d, plane)
        pl.semaphore_signal(barrier, inc=1, device_id=(t // 2, 2 * z + t % 2), device_id_type=MESH)
    for d in range(1, zs):
        t = lax.rem(z + d, zs)
        pl.semaphore_signal(barrier, inc=1, device_id=(row, 2 * t + core), device_id_type=MESH)
    pl.semaphore_wait(barrier, plane - 1 + zs - 1)

    pending = []

    def send(src, dst, ssem, rsem, dev):
        return pltpu.make_async_remote_copy(
            src_ref=src, dst_ref=dst, send_sem=ssem, recv_sem=rsem, device_id=dev, device_id_type=MESH
        )

    def rs_copies(u, src):
        out = []
        for d in range(1, rows):
            t = lax.rem(row + d, rows)
            out.append(send(src.at[t], rsbuf.at[u, d - 1], rs_send.at[u, d - 1], rs_recv.at[u, d - 1], (t, col)))
        return out

    def rs_start(u, src):
        for copy in rs_copies(u, src):
            copy.start()

    def rs_finish(u, src):
        total = src[row]
        for d, copy in enumerate(rs_copies(u, src)):
            copy.wait_recv()
            total = total + rsbuf[u, d]
        for copy in rs_copies(u, src):
            copy.wait_send()
        return total

    def up_copy(u, s):
        return send(zbuf.at[u, s], zbuf.at[u, s], up_send.at[u, s], up_recv.at[u, s], (row, col + 2))

    def dn_copy(u, s):
        return send(zbuf.at[u, s], zbuf.at[u, s], dn_send.at[u, s], dn_recv.at[u, s], (row, col - 2))

    def plane_copy(u, t, slot, d):
        return send(zbuf.at[u, t], rowbuf.at[u, slot], pl_send.at[u, d], pl_recv.at[u, d], (t, col))

    def slot_of(k, r):
        return k * rows + r

    def to_plane(u, s):
        @pl.when(s != row)
        def _():
            plane_copy(u, s, slot_of(core, row), lax.rem(s - row + rows, rows)).start()

        @pl.when(s == row)
        def _():
            pltpu.make_async_copy(zbuf.at[u, s], rowbuf.at[u, slot_of(core, row)], own_sem.at[u]).start()

    def spread_start(u, piece):
        zbuf[u, z] = piece

        @pl.when(z + 1 < zs)
        def _():
            up_copy(u, z).start()

        @pl.when(z > 0)
        def _():
            dn_copy(u, z).start()

        to_plane(u, z)

    def spread_step(u, s):
        low, high = z - s, z + s

        @pl.when(low >= 0)
        def _():
            up_copy(u, low).wait_recv()

            @pl.when(z + 1 < zs)
            def _():
                up_copy(u, low).start()

            to_plane(u, low)

        @pl.when(high < zs)
        def _():
            dn_copy(u, high).wait_recv()

            @pl.when(z > 0)
            def _():
                dn_copy(u, high).start()

            to_plane(u, high)

    def partner_copy(u, d):
        slot = slot_of(core, lax.rem(row - d + rows, rows))
        return send(rowbuf.at[u, slot], rowbuf.at[u, slot], dd_send.at[u, d], dd_recv.at[u, d], (row, col + 1 - 2 * core))

    def spread_half(u):
        pltpu.make_async_copy(zbuf.at[u, row], rowbuf.at[u, slot_of(core, row)], own_sem.at[u]).wait()
        partner_copy(u, 0).start()
        for d in range(1, rows):
            plane_copy(u, row, slot_of(core, row), d).wait_recv()
            partner_copy(u, d).start()

    def spread_rest(u):
        for d in range(rows):
            partner_copy(u, d).wait_recv()

    def spread_drain(u):
        for d in range(rows):
            partner_copy(u, d).wait_send()
        for d in range(1, rows):
            plane_copy(u, row, slot_of(core, row), d).wait_send()

        for s in range(zs):
            @pl.when((z + 1 < zs) & (z >= s))
            def _():
                up_copy(u, s).wait_send()

            @pl.when((z > 0) & (z <= s))
            def _():
                dn_copy(u, s).wait_send()

    def ar_refs(u, m):
        deep = width * m // plane
        return deep, pl.ds(0, deep)

    def ar_one(u, m, d):
        deep, span = ar_refs(u, m)
        t = lax.rem(q + d, plane)
        return send(
            a_loc.at[u, t, span], a_in.at[u, d - 1, span], a_s1.at[u, d - 1], a_r1.at[u, d - 1], (t // 2, 2 * z + t % 2)
        )

    def ar_two(u, m, d):
        deep, span = ar_refs(u, m)
        t = lax.rem(z + d, zs)
        return send(
            a_z.at[u, z, span], a_z.at[u, z, span], a_s2.at[u, d - 1], a_r2.at[u, d - 1], (row, 2 * t + core)
        )

    def ar_three(u, m, d):
        deep, span = ar_refs(u, m)
        t = lax.rem(q + d, plane)
        return send(
            a_full.at[u, q, span], a_full.at[u, q, span], a_s3.at[u, d - 1], a_r3.at[u, d - 1],
            (t // 2, 2 * z + t % 2),
        )

    def ar_start(u, m, value):
        deep, span = ar_refs(u, m)
        for t in range(plane):
            a_loc[u, t, span] = value[t * deep : (t + 1) * deep]
        for d in range(1, plane):
            ar_one(u, m, d).start()

    def ar_mid(u, m):
        deep, span = ar_refs(u, m)
        total = a_loc[u, q, span]
        for d in range(1, plane):
            ar_one(u, m, d).wait_recv()
            total = total + a_in[u, d - 1, span]
        a_z[u, z, span] = total
        for d in range(1, zs):
            ar_two(u, m, d).start()

    def ar_late(u, m):
        deep, span = ar_refs(u, m)
        for d in range(1, zs):
            ar_two(u, m, d).wait_recv()
        total = a_z[u, 0, span]
        for s in range(1, zs):
            total = total + a_z[u, s, span]
        a_full[u, q, span] = total
        for d in range(1, plane):
            ar_three(u, m, d).start()

    def ar_finish(u, m):
        deep, span = ar_refs(u, m)
        for d in range(1, plane):
            ar_three(u, m, d).wait_recv()
        value = jnp.concatenate([a_full[u, t, span] for t in range(plane)], axis=0)
        for d in range(1, plane):
            ar_one(u, m, d).wait_send()
            ar_three(u, m, d).wait_send()
        for d in range(1, zs):
            ar_two(u, m, d).wait_send()
        return value

    def all_sum(u, m, value):
        ar_start(u, m, value)
        ar_mid(u, m)
        ar_late(u, m)
        return ar_finish(u, m)

    deep = stage.shape[1]
    chunks = cov_ref.shape[0] // deep

    def fetch(i):
        return pltpu.make_async_copy(cov_ref.at[pl.ds(i * deep, deep), :], stage.at[i % 2], stage_sem.at[i % 2])

    def load_covariance():
        def chunk(i, carry):
            @pl.when(i + 1 < chunks)
            def _():
                fetch(i + 1).start()

            fetch(i).wait()

            def split(s, inner):
                for n in range(rows):
                    high, low = halves(stage[i % 2, pl.ds(s * 16, 16), n * wide : (n + 1) * wide])
                    ahi[n, pl.ds(i * deep + s * 16, 16), :] = high
                    alo[n, pl.ds(i * deep + s * 16, 16), :] = low
                return inner

            lax.fori_loop(0, deep // 16, split, 0, unroll=2)
            return carry

        lax.fori_loop(0, chunks, chunk, 0)

    def multiply(u, first, j):
        high, low = halves(rowbuf[u, j])
        both = jnp.concatenate([high, low], axis=0)

        def column(n, carry):
            span = pl.ds(pl.multiple_of(j * wide, wide), wide)
            go = functools.partial(lax.dot_general, dimension_numbers=NN, preferred_element_type=F32)
            one = go(both, ahi[n, span, :])
            two = go(high, alo[n, span, :])
            value = one[:width] + one[width:] + two
            part[u, n] = jnp.where(first, value, value + part[u, n])
            return carry

        lax.fori_loop(0, rows, column, 0)

    def product(u):
        lax.fori_loop(0, rows, lambda i, c: (multiply(u, i == 0, core * rows + i), c)[1], 0)
        spread_rest(u)
        lax.fori_loop(0, rows, lambda i, c: (multiply(u, False, (1 - core) * rows + i), c)[1], 0)

    def spread_wait(u):
        for s in range(1, zs):
            spread_step(u, s)
        spread_half(u)

    fetch(0).start()
    rs_start(0, x_ref)
    part[0] = jnp.zeros(part.shape[1:], F32)
    part[1] = jnp.zeros(part.shape[1:], F32)
    load_covariance()
    start = rs_finish(0, x_ref)
    spread_start(0, start)
    gram = all_sum(0, 1, dot(start, start, NT))
    upper0, inv0 = factor(gram, work)
    small_ref[0] = upper0
    small_ref[1] = inv0
    q0 = dot(inv0, start, NN)
    spread_wait(0)
    product(0)
    rs_start(1, part.at[0])
    image = rs_finish(1, part.at[0])
    image0 = dot(inv0, image, NN)
    h1 = all_sum(1, 1, dot(q0, image0, NT))
    once = image0 - dot(h1, q0, TN)
    spread_start(1, once)
    both = all_sum(2, 2, jnp.concatenate([dot(q0, once, NT), dot(once, once, NT)], axis=0))
    h2, raw = both[:width], both[width:]
    gram = raw - dot(h2, h2, TN)
    upper1, inv1 = factor(gram, work)
    small_ref[2] = h1
    small_ref[3] = h2
    small_ref[4] = upper1
    small_ref[5] = inv1
    twice = once - dot(h2, q0, TN)
    q1 = dot(inv1, twice, NN)
    spread_wait(1)
    product(1)
    rs_start(2, part.at[1])
    image = rs_finish(2, part.at[1])
    image1 = dot(inv1, image - dot(h2, image0, TN), NN)
    spread_start(2, image1)
    stacked = jnp.concatenate([q0, q1], axis=0)
    g1 = all_sum(3, 2, dot(stacked, image1, NT))
    once = image1 - dot(g1, stacked, TN)
    both = all_sum(4, 3, jnp.concatenate([dot(stacked, once, NT), dot(once, once, NT)], axis=0))
    g2, raw = both[: 2 * width], both[2 * width :]
    gram = raw - dot(g2, g2, TN)
    spread_wait(2)
    upper2, inv2 = factor(gram, work)
    small_ref[6] = g1[:width]
    small_ref[7] = g1[width:]
    small_ref[8] = g2[:width]
    small_ref[9] = g2[width:]
    small_ref[10] = upper2
    small_ref[11] = inv2
    spread_rest(2)
    for u in range(3):
        pltpu.make_async_copy(rowbuf.at[u], wide_ref.at[u], out_sem.at[u]).start()
    for u in range(3):
        spread_drain(u)
    for u in range(3):
        pltpu.make_async_copy(rowbuf.at[u], wide_ref.at[u], out_sem.at[u]).wait()


def main(rows, cols, x, covariance):
    row_count, col_count = covariance.shape
    width, wide = x.shape[1:]
    zs, plane = cols // 2, 2 * rows
    deep = min(256, row_count)
    dma = pltpu.SemaphoreType.DMA
    uses = 3
    sums, most = 5, 3 * width // plane
    return pl.pallas_call(
        functools.partial(main_kernel, rows, cols),
        out_shape=(
            jax.ShapeDtypeStruct((3, cols, width, wide), F32),
            jax.ShapeDtypeStruct((12, width, width), F32),
        ),
        in_specs=[pl.BlockSpec(memory_space=pltpu.VMEM), pl.BlockSpec(memory_space=pl.ANY)],
        out_specs=(pl.BlockSpec(memory_space=pl.ANY), pl.BlockSpec(memory_space=pltpu.VMEM)),
        scratch_shapes=[
            pltpu.VMEM((rows, row_count, wide), BF16),
            pltpu.VMEM((rows, row_count, wide), BF16),
            pltpu.VMEM((2, deep, col_count), F32),
            dma((2,)),
            pltpu.VMEM((2, rows, width, wide), F32),
            pltpu.VMEM((uses, rows - 1, width, wide), F32),
            dma((uses, rows - 1)), dma((uses, rows - 1)),
            pltpu.VMEM((uses, zs, width, wide), F32),
            dma((uses, zs)), dma((uses, zs)), dma((uses, zs)), dma((uses, zs)),
            pltpu.VMEM((uses, cols, width, wide), F32),
            dma((uses, rows)), dma((uses, rows)), dma((uses, rows)), dma((uses, rows)), dma((uses,)), dma((uses,)),
            pltpu.VMEM((sums, plane, most, width), F32),
            pltpu.VMEM((sums, plane - 1, most, width), F32),
            pltpu.VMEM((sums, zs, most, width), F32),
            pltpu.VMEM((sums, plane, most, width), F32),
            dma((sums, plane - 1)), dma((sums, plane - 1)),
            dma((sums, zs - 1)), dma((sums, zs - 1)),
            dma((sums, plane - 1)), dma((sums, plane - 1)),
            pltpu.VMEM((width, 2 * width), F32),
        ],
        compiler_params=pltpu.CompilerParams(collective_id=0, has_side_effects=True, vmem_limit_bytes=LIMIT),
        name="lanczos",
    )(x, covariance)


def finish_kernel(root, wide_ref, small_ref, basis_ref, projection_ref, first_ref):
    width = small_ref.shape[1]
    get = lambda i: small_ref[i]
    upper0, inv0, h1, h2, upper1, inv1, g1a, g1b, g2a, g2b, upper2, inv2 = [get(i) for i in range(12)]
    q0 = dot3(inv0, wide_ref[0, 0], NN)
    q1 = dot3(inv1, wide_ref[1, 0] - dot3(h2, q0, TN), NN)
    stacked = jnp.concatenate([q0, q1], axis=0)
    once = wide_ref[2, 0] - dot3(jnp.concatenate([g1a, g1b], axis=0), stacked, TN)
    twice = once - dot3(jnp.concatenate([g2a, g2b], axis=0), stacked, TN)
    q2 = dot3(inv2, twice, NN)
    for i, value in enumerate((q0, q1, q2)):
        basis_ref[:, i * width : (i + 1) * width] = value.T * root

    @pl.when(pl.program_id(0) == 0)
    def _():
        zero = jnp.zeros((width, width), F32)
        spot = lambda i: pl.ds(i * width, width)
        for r, c, value in (
            (0, 0, h1 + h2), (1, 0, upper1), (2, 0, zero),
            (0, 1, g1a + g2a), (1, 1, g1b + g2b), (2, 1, upper2),
        ):
            projection_ref[spot(r), spot(c)] = value
        for r, c, value in ((0, 0, h1), (1, 0, zero), (2, 0, zero), (0, 1, g1a), (1, 1, g1b), (2, 1, zero)):
            first_ref[spot(r), spot(c)] = value


def finish(order, wide_blocks, small):
    _, cols, width, wide = wide_blocks.shape
    whole = lambda i: (0, 0)
    return pl.pallas_call(
        functools.partial(finish_kernel, float(order) ** 0.5),
        grid=(cols,),
        out_shape=(
            jax.ShapeDtypeStruct((cols * wide, 3 * width), F32),
            jax.ShapeDtypeStruct((3 * width, 2 * width), F32),
            jax.ShapeDtypeStruct((3 * width, 2 * width), F32),
        ),
        in_specs=[
            pl.BlockSpec((3, 1, width, wide), lambda i: (0, i, 0, 0)),
            pl.BlockSpec(small.shape, lambda i: (0, 0, 0)),
        ],
        out_specs=(
            pl.BlockSpec((wide, 3 * width), lambda i: (i, 0)),
            pl.BlockSpec((3 * width, 2 * width), whole),
            pl.BlockSpec((3 * width, 2 * width), whole),
        ),
        compiler_params=pltpu.CompilerParams(vmem_limit_bytes=32 * 1024 * 1024),
        name="finish",
    )(wide_blocks, small)


def solve(rows, cols, covariance, seed_index):
    x = gather(rows, covariance, seed_index)
    wide_blocks, small = main(rows, cols, x, covariance)
    return finish(rows * covariance.shape[0], wide_blocks, small)


def solution(mesh):
    rows, cols = mesh.shape["row"], mesh.shape["col"]
    return jax.shard_map(
        lambda covariance, seed_index: solve(rows, cols, covariance, seed_index),
        mesh=mesh,
        in_specs=(P("row", "col"), P()),
        out_specs=(P("row", None), P(), P()),
        check_vma=False,
    )
```

```python
import functools

import jax
import jax.numpy as jnp
from jax import lax
from jax.experimental import pallas as pl
from jax.experimental.pallas import tpu as pltpu
from jax.sharding import PartitionSpec as P

MESH = pl.DeviceIdType.MESH
F32, BF16 = jnp.float32, jnp.bfloat16
PARTS = 2
LIMIT = 66 * 1024 * 1024 - 2 * 1024 * 1024

NN = (((1,), (0,)), ((), ()))
NT = (((1,), (1,)), ((), ()))
TN = (((0,), (0,)), ((), ()))


def dot(left, right, dims):
    return lax.dot_general(left, right, dims, precision=lax.Precision.HIGHEST, preferred_element_type=F32)


def halves(value):
    high = value.astype(BF16)
    return high, (value - high.astype(F32)).astype(BF16)


def dot3(left, right, dims):
    lh, ll = halves(left)
    rh, rl = halves(right)
    go = functools.partial(lax.dot_general, dimension_numbers=dims, preferred_element_type=F32)
    return go(lh, rh) + (go(lh, rl) + go(ll, rh))


def gather_kernel(rows, index_ref, inside_ref, cov_ref, out_ref, buf, sem):
    width, cols = buf.shape
    wide = cols // rows

    def fetch(i, carry):
        pltpu.make_async_copy(cov_ref.at[pl.ds(index_ref[i], 1), :], buf.at[pl.ds(i, 1), :], sem).start()
        return carry

    lax.fori_loop(0, width, fetch, 0, unroll=8)
    pltpu.make_async_copy(cov_ref.at[pl.ds(0, width), :], buf, sem).wait()
    keep = inside_ref[...] > 0
    for n in range(rows):
        out_ref[n] = jnp.where(keep, buf[:, n * wide : (n + 1) * wide], 0.0)


def gather(rows, covariance, seed_index):
    row_count, cols = covariance.shape
    width = seed_index.shape[0]
    offsets = seed_index - lax.axis_index("row") * row_count
    inside = (offsets >= 0) & (offsets < row_count)
    return pl.pallas_call(
        functools.partial(gather_kernel, rows),
        out_shape=jax.ShapeDtypeStruct((rows, width, cols // rows), F32),
        in_specs=[
            pl.BlockSpec(memory_space=pltpu.SMEM),
            pl.BlockSpec(memory_space=pltpu.VMEM),
            pl.BlockSpec(memory_space=pl.ANY),
        ],
        out_specs=pl.BlockSpec(memory_space=pltpu.VMEM),
        scratch_shapes=[pltpu.VMEM((width, cols), F32), pltpu.SemaphoreType.DMA],
        compiler_params=pltpu.CompilerParams(vmem_limit_bytes=LIMIT),
        name="gather",
    )(jnp.clip(offsets, 0, row_count - 1), inside.astype(jnp.int32)[:, None], covariance)


def factor(gram, work):
    width = gram.shape[0]
    deep = 8
    down = lax.broadcasted_iota(jnp.int32, (width, width), 0)
    across = lax.broadcasted_iota(jnp.int32, (width, width), 1)
    few = lax.broadcasted_iota(jnp.int32, (deep, width), 1)
    tall = lax.broadcasted_iota(jnp.int32, (width, 1), 0)
    short = lax.broadcasted_iota(jnp.int32, (deep, 1), 0)
    work[:, :width] = gram
    work[:, width:] = jnp.where(down == across, 1.0, 0.0)

    def panel(p, carry):
        base = pl.multiple_of(p * deep, deep)
        block = work[pl.ds(base, deep), :]
        now = work[...]
        left, top = now[:, :width], block[:, :width]
        small = [jnp.sum(jnp.where(few == base + t, top, 0.0), axis=1, keepdims=True) for t in range(deep)]
        large = [jnp.sum(jnp.where(across == base + t, left, 0.0), axis=1, keepdims=True) for t in range(deep)]
        for t in range(deep):
            pivot = small[t][t : t + 1]
            scale = lax.rsqrt(pivot)
            scale = scale * (1.5 - 0.5 * pivot * scale * scale)
            unit = block[t : t + 1] * scale
            column = small[t] * scale
            large[t] = large[t] * scale
            for e in range(t + 1, deep):
                factor_e = column[e : e + 1]
                small[e] = small[e] - column * factor_e
                large[e] = large[e] - large[t] * factor_e
            block = jnp.where(short == t, unit, block - jnp.where(short > t, column, 0.0) * unit)
        for t in range(deep):
            now = now - jnp.where(tall >= base + deep, large[t], 0.0) * block[t : t + 1]
        work[...] = now
        work[pl.ds(base, deep), :] = block
        return carry

    lax.fori_loop(0, width // deep, panel, 0)
    upper = jnp.where(down <= across, work[:, :width], 0.0)
    return upper, work[:, width:]


def main_kernel(
    rows, cols, x_ref, cov_ref,
    wide_ref, small_ref,
    ahi, alo, stage, stage_sem, part, rsbuf, rs_send, rs_recv,
    zbuf, up_send, up_recv, dn_send, dn_recv, rowbuf, pl_send, pl_recv, dd_send, dd_recv, own_sem, out_sem,
    a_loc, a_in, a_z, a_full, a_s1, a_r1, a_s2, a_r2, a_s3, a_r3, work, wsplit,
):
    zs = cols // 2
    width, wide = x_ref.shape[1], x_ref.shape[2]
    row = lax.axis_index("row")
    col = lax.axis_index("col")
    z = col // 2
    core = col % 2
    plane = 2 * rows
    q = row * 2 + core

    deep = stage.shape[1]
    chunks = cov_ref.shape[0] // deep

    def fetch(i):
        return pltpu.make_async_copy(cov_ref.at[pl.ds(i * deep, deep), :], stage.at[i % 2], stage_sem.at[i % 2])

    fetch(0).start()
    barrier = pltpu.get_barrier_semaphore()
    for d in range(1, plane):
        t = lax.rem(q + d, plane)
        pl.semaphore_signal(barrier, inc=1, device_id=(t // 2, 2 * z + t % 2), device_id_type=MESH)
    for d in range(1, zs):
        t = lax.rem(z + d, zs)
        pl.semaphore_signal(barrier, inc=1, device_id=(row, 2 * t + core), device_id_type=MESH)
    pl.semaphore_wait(barrier, plane - 1 + zs - 1)

    pending = []

    def send(src, dst, ssem, rsem, dev):
        return pltpu.make_async_remote_copy(
            src_ref=src, dst_ref=dst, send_sem=ssem, recv_sem=rsem, device_id=dev, device_id_type=MESH
        )

    def rs_copy(u, src, d):
        t = lax.rem(row + d, rows)
        return send(src.at[t], rsbuf.at[u, d - 1], rs_send.at[u, d - 1], rs_recv.at[u, d - 1], (t, col))

    def rs_copies(u, src):
        return [rs_copy(u, src, d) for d in range(1, rows)]

    def rs_start(u, src):
        for copy in rs_copies(u, src):
            copy.start()


    def rs_finish(u, src):
        total = src[row]
        for d, copy in enumerate(rs_copies(u, src)):
            copy.wait_recv()
            total = total + rsbuf[u, d]
        for copy in rs_copies(u, src):
            copy.wait_send()
        return total

    parts = up_send.shape[2]
    thick = width // parts

    def part_of(h):
        return pl.ds(h * thick, thick)

    def up_copy(u, s, h):
        ref = zbuf.at[u, s, part_of(h)]
        return send(ref, ref, up_send.at[u, s, h], up_recv.at[u, s, h], (row, col + 2))

    def dn_copy(u, s, h):
        ref = zbuf.at[u, s, part_of(h)]
        return send(ref, ref, dn_send.at[u, s, h], dn_recv.at[u, s, h], (row, col - 2))

    def slot_of(k, r):
        return k * rows + r

    def plane_copy(u, t, h, d):
        dst = rowbuf.at[u, slot_of(core, row), part_of(h)]
        return send(zbuf.at[u, t, part_of(h)], dst, pl_send.at[u, d, h], pl_recv.at[u, d, h], (t, col))

    def own_copy(u):
        return pltpu.make_async_copy(zbuf.at[u, row], rowbuf.at[u, slot_of(core, row)], own_sem.at[u])

    def to_plane(u, s, h):
        @pl.when(s != row)
        def _():
            plane_copy(u, s, h, lax.rem(s - row + rows, rows)).start()

        if h == parts - 1:
            @pl.when(s == row)
            def _():
                own_copy(u).start()

    def spread_start(u, piece):
        zbuf[u, z] = piece
        for h in range(parts):
            @pl.when(z + 1 < zs)
            def _():
                up_copy(u, z, h).start()

            @pl.when(z > 0)
            def _():
                dn_copy(u, z, h).start()

            to_plane(u, z, h)

    def spread_step(u, s):
        low, high = z - s, z + s
        for h in range(parts):
            @pl.when(low >= 0)
            def _():
                up_copy(u, low, h).wait_recv()

                @pl.when(z + 1 < zs)
                def _():
                    up_copy(u, low, h).start()

                to_plane(u, low, h)

            @pl.when(high < zs)
            def _():
                dn_copy(u, high, h).wait_recv()

                @pl.when(z > 0)
                def _():
                    dn_copy(u, high, h).start()

                to_plane(u, high, h)

    def partner_copy(u, d, h):
        ref = rowbuf.at[u, slot_of(core, lax.rem(row - d + rows, rows)), part_of(h)]
        return send(ref, ref, dd_send.at[u, d, h], dd_recv.at[u, d, h], (row, col + 1 - 2 * core))

    def spread_half(u):
        own_copy(u).wait()
        for h in range(parts):
            partner_copy(u, 0, h).start()
        for h in range(parts):
            for d in range(1, rows):
                plane_copy(u, row, h, d).wait_recv()
                partner_copy(u, d, h).start()

    def spread_rest(u):
        for h in range(parts):
            for d in range(rows):
                partner_copy(u, d, h).wait_recv()

    def spread_drain(u):
        for h in range(parts):
            for d in range(rows):
                partner_copy(u, d, h).wait_send()
            for d in range(1, rows):
                plane_copy(u, row, h, d).wait_send()
            for s in range(zs):
                @pl.when((z + 1 < zs) & (z >= s))
                def _():
                    up_copy(u, s, h).wait_send()

                @pl.when((z > 0) & (z <= s))
                def _():
                    dn_copy(u, s, h).wait_send()

    def ar_refs(u, m):
        deep = width * m // plane
        return deep, pl.ds(0, deep)

    def ar_one(u, m, d):
        deep, span = ar_refs(u, m)
        t = lax.rem(q + d, plane)
        return send(
            a_loc.at[u, t, span], a_in.at[u, d - 1, span], a_s1.at[u, d - 1], a_r1.at[u, d - 1], (t // 2, 2 * z + t % 2)
        )

    def ar_two(u, m, d):
        deep, span = ar_refs(u, m)
        t = lax.rem(z + d, zs)
        return send(
            a_z.at[u, z, span], a_z.at[u, z, span], a_s2.at[u, d - 1], a_r2.at[u, d - 1], (row, 2 * t + core)
        )

    def ar_three(u, m, d):
        deep, span = ar_refs(u, m)
        t = lax.rem(q + d, plane)
        return send(
            a_full.at[u, q, span], a_full.at[u, q, span], a_s3.at[u, d - 1], a_r3.at[u, d - 1],
            (t // 2, 2 * z + t % 2),
        )

    def ar_start(u, m, value):
        deep, span = ar_refs(u, m)
        for t in range(plane):
            a_loc[u, t, span] = value[t * deep : (t + 1) * deep]
        for d in range(1, plane):
            ar_one(u, m, d).start()

    def ar_mid(u, m):
        deep, span = ar_refs(u, m)
        total = a_loc[u, q, span]
        for d in range(1, plane):
            ar_one(u, m, d).wait_recv()
            total = total + a_in[u, d - 1, span]
        a_z[u, z, span] = total
        for d in range(1, zs):
            ar_two(u, m, d).start()

    def ar_late(u, m):
        deep, span = ar_refs(u, m)
        for d in range(1, zs):
            ar_two(u, m, d).wait_recv()
        total = a_z[u, 0, span]
        for s in range(1, zs):
            total = total + a_z[u, s, span]
        a_full[u, q, span] = total
        for d in range(1, plane):
            ar_three(u, m, d).start()

    def ar_finish(u, m):
        deep, span = ar_refs(u, m)
        for d in range(1, plane):
            ar_three(u, m, d).wait_recv()
        value = jnp.concatenate([a_full[u, t, span] for t in range(plane)], axis=0)
        for d in range(1, plane):
            ar_one(u, m, d).wait_send()
            ar_three(u, m, d).wait_send()
        for d in range(1, zs):
            ar_two(u, m, d).wait_send()
        return value

    def all_sum(u, m, value):
        ar_start(u, m, value)
        ar_mid(u, m)
        ar_late(u, m)
        return ar_finish(u, m)

    def load_covariance(begin, end):
        def chunk(i, carry):
            @pl.when(i + 1 < chunks)
            def _():
                fetch(i + 1).start()

            fetch(i).wait()

            def split(s, inner):
                for n in range(rows):
                    high, low = halves(stage[i % 2, pl.ds(s * 16, 16), n * wide : (n + 1) * wide])
                    ahi[n, pl.ds(i * deep + s * 16, 16), :] = high
                    alo[n, pl.ds(i * deep + s * 16, 16), :] = low
                return inner

            lax.fori_loop(0, deep // 16, split, 0, unroll=4)
            return carry

        lax.fori_loop(begin, end, chunk, 0)

    def term(n, span, high, both):
        go = functools.partial(lax.dot_general, dimension_numbers=NN, preferred_element_type=F32)
        one = go(both, ahi[n, span, :])
        two = go(high, alo[n, span, :])
        return one[:width] + one[width:] + two

    def split_rows(u, j):
        high, low = halves(rowbuf[u, j])
        wsplit[j, :width] = high
        wsplit[j, width:] = low

    def span_of(j):
        return pl.ds(pl.multiple_of(j * wide, wide), wide)

    def product_near(u):
        def piece(i, carry):
            j = core * rows + i
            split_rows(u, j)
            for n in range(rows):
                value = term(n, span_of(j), wsplit[j, :width], wsplit[j])
                part[u, n] = jnp.where(i == 0, value, value + part[u, n])
            return carry

        lax.fori_loop(0, rows, piece, 0)

    def product_far(u, rs):
        lax.fori_loop(0, rows, lambda i, c: (split_rows(u, (1 - core) * rows + i), c)[1], 0)

        def target(d, carry):
            n = lax.rem(row + d, rows)
            value = part[u, n]
            for i in range(rows):
                j = (1 - core) * rows + i
                value = value + term(n, span_of(j), wsplit[j, :width], wsplit[j])
            part[u, n] = value

            @pl.when(d < rows)
            def _():
                rs_copy(rs, part.at[u], d).start()

            return carry

        lax.fori_loop(1, rows + 1, target, 0)

    def scope(name):
        return jax.named_scope(name)

    def rows_to_basis(u, inverse, other):
        def piece(j, carry):
            value = rowbuf[u, j]
            if other is not None:
                value = value - dot3(other, rowbuf[0, j], TN)
            rowbuf[u, j] = dot3(inverse, value, NN)
            return carry

        lax.fori_loop(0, cols, piece, 0)
        wide_copy(u).start()

    def wide_copy(u):
        return pltpu.make_async_copy(rowbuf.at[u], wide_ref.at[u], out_sem.at[u])

    def spread_and_multiply(u, block, a, m, small):
        with scope(f"spread_start#{u}"):
            spread_start(u, block)
            ar_start(a, m, small())
        if u == 0:
            with scope("load_rest#0"):
                load_covariance(chunks // 2, chunks)
        with scope(f"spread_step#{u}"):
            for s in range(1, zs):
                spread_step(u, s)
        with scope(f"spread_half#{u}"):
            ar_mid(a, m)
            spread_half(u)
        with scope(f"near#{u}"):
            product_near(u)
        with scope(f"spread_rest#{u}"):
            ar_late(a, m)
            spread_rest(u)
        with scope(f"far#{u}"):
            product_far(u, u + 1)

    with scope("start#0"):
        rs_start(0, x_ref)
        load_covariance(0, chunks // 2)
    with scope("rs#0"):
        start = rs_finish(0, x_ref)
    spread_and_multiply(0, start, 0, 1, lambda: dot(start, start, NT))
    with scope("factor#0"):
        gram = ar_finish(0, 1)
        upper0, inv0 = factor(gram, work)
        small_ref[0] = upper0
        small_ref[1] = inv0
        q0 = dot(inv0, start, NN)
    with scope("rs#1"):
        image = rs_finish(1, part.at[0])
    with scope("sum#1"):
        image0 = dot(inv0, image, NN)
        ar_start(1, 1, dot(q0, image0, NT))
        ar_mid(1, 1)
        ar_late(1, 1)
        h1 = ar_finish(1, 1)
        once = image0 - dot(h1, q0, TN)
    spread_and_multiply(
        1, once, 2, 2, lambda: jnp.concatenate([dot(q0, once, NT), dot(once, once, NT)], axis=0)
    )
    with scope("factor#1"):
        both = ar_finish(2, 2)
        h2, raw = both[:width], both[width:]
        gram = raw - dot(h2, h2, TN)
        upper1, inv1 = factor(gram, work)
        small_ref[2] = h1
        small_ref[3] = h2
        small_ref[4] = upper1
        small_ref[5] = inv1
        twice = once - dot(h2, q0, TN)
        q1 = dot(inv1, twice, NN)
        shift = dot(h2, image0, TN)
        stacked = jnp.concatenate([q0, q1], axis=0)
    with scope("rs#2"):
        image = rs_finish(2, part.at[1])
    with scope("sum#3"):
        image1 = dot(inv1, image - shift, NN)
        ar_start(3, 2, dot(stacked, image1, NT))
        spread_drain(0)
        rows_to_basis(0, inv0, None)
        ar_mid(3, 2)
        ar_late(3, 2)
        g1 = ar_finish(3, 2)
        once = image1 - dot(g1, stacked, TN)
    with scope("last_start#0"):
        ar_start(4, 3, jnp.concatenate([dot(stacked, once, NT), dot(once, once, NT)], axis=0))
        spread_start(2, once)
    with scope("basis#1"):
        spread_drain(1)
        wide_copy(0).wait()
        rows_to_basis(1, inv1, h2)
    with scope("last_steps#0"):
        spread_step(2, 1)
        ar_mid(4, 3)
        for s in range(2, zs):
            spread_step(2, s)
        ar_late(4, 3)
    with scope("last_half#0"):
        spread_half(2)
    with scope("last_sum#0"):
        both = ar_finish(4, 3)
    with scope("factor#2"):
        g2, raw = both[: 2 * width], both[2 * width :]
        gram = raw - dot(g2, g2, TN)
        upper2, inv2 = factor(gram, work)
        small_ref[6] = g1[:width]
        small_ref[7] = g1[width:]
        small_ref[8] = g2[:width]
        small_ref[9] = g2[width:]
        small_ref[10] = upper2
        small_ref[11] = inv2
    with scope("end#0"):
        spread_rest(2)
        wide_copy(2).start()
        spread_drain(2)
        wide_copy(1).wait()
        wide_copy(2).wait()


def main(rows, cols, x, covariance):
    row_count, col_count = covariance.shape
    width, wide = x.shape[1:]
    zs, plane = cols // 2, 2 * rows
    deep = min(256, row_count)
    dma = pltpu.SemaphoreType.DMA
    uses = 3
    sums, most = 5, 3 * width // plane
    return pl.pallas_call(
        functools.partial(main_kernel, rows, cols),
        out_shape=(
            jax.ShapeDtypeStruct((3, cols, width, wide), F32),
            jax.ShapeDtypeStruct((12, width, width), F32),
        ),
        in_specs=[pl.BlockSpec(memory_space=pltpu.VMEM), pl.BlockSpec(memory_space=pl.ANY)],
        out_specs=(pl.BlockSpec(memory_space=pl.ANY), pl.BlockSpec(memory_space=pltpu.VMEM)),
        scratch_shapes=[
            pltpu.VMEM((rows, row_count, wide), BF16),
            pltpu.VMEM((rows, row_count, wide), BF16),
            pltpu.VMEM((2, deep, col_count), F32),
            dma((2,)),
            pltpu.VMEM((2, rows, width, wide), F32),
            pltpu.VMEM((uses, rows - 1, width, wide), F32),
            dma((uses, rows - 1)), dma((uses, rows - 1)),
            pltpu.VMEM((uses, zs, width, wide), F32),
            dma((uses, zs, PARTS)), dma((uses, zs, PARTS)), dma((uses, zs, PARTS)), dma((uses, zs, PARTS)),
            pltpu.VMEM((uses, cols, width, wide), F32),
            dma((uses, rows, PARTS)), dma((uses, rows, PARTS)), dma((uses, rows, PARTS)), dma((uses, rows, PARTS)),
            dma((uses,)), dma((uses,)),
            pltpu.VMEM((sums, plane, most, width), F32),
            pltpu.VMEM((sums, plane - 1, most, width), F32),
            pltpu.VMEM((sums, zs, most, width), F32),
            pltpu.VMEM((sums, plane, most, width), F32),
            dma((sums, plane - 1)), dma((sums, plane - 1)),
            dma((sums, zs - 1)), dma((sums, zs - 1)),
            dma((sums, plane - 1)), dma((sums, plane - 1)),
            pltpu.VMEM((width, 2 * width), F32),
            pltpu.VMEM((cols, 2 * width, wide), BF16),
        ],
        compiler_params=pltpu.CompilerParams(collective_id=0, has_side_effects=True, vmem_limit_bytes=LIMIT),
        name="lanczos",
    )(x, covariance)


def finish_kernel(root, wide_ref, small_ref, basis_ref, projection_ref, first_ref):
    width = small_ref.shape[1]
    get = lambda i: small_ref[i]
    upper0, inv0, h1, h2, upper1, inv1, g1a, g1b, g2a, g2b, upper2, inv2 = [get(i) for i in range(12)]
    q0, q1 = wide_ref[0, 0], wide_ref[1, 0]
    q2 = dot3(inv2, wide_ref[2, 0] - (dot3(g2a, q0, TN) + dot3(g2b, q1, TN)), NN)
    for i, value in enumerate((q0, q1, q2)):
        basis_ref[:, i * width : (i + 1) * width] = value.T * root

    @pl.when(pl.program_id(0) == 0)
    def _():
        zero = jnp.zeros((width, width), F32)
        spot = lambda i: pl.ds(i * width, width)
        for r, c, value in (
            (0, 0, h1 + h2), (1, 0, upper1), (2, 0, zero),
            (0, 1, g1a + g2a), (1, 1, g1b + g2b), (2, 1, upper2),
        ):
            projection_ref[spot(r), spot(c)] = value
        for r, c, value in ((0, 0, h1), (1, 0, zero), (2, 0, zero), (0, 1, g1a), (1, 1, g1b), (2, 1, zero)):
            first_ref[spot(r), spot(c)] = value


def finish(order, wide_blocks, small):
    _, cols, width, wide = wide_blocks.shape
    whole = lambda i: (0, 0)
    return pl.pallas_call(
        functools.partial(finish_kernel, float(order) ** 0.5),
        grid=(cols,),
        out_shape=(
            jax.ShapeDtypeStruct((cols * wide, 3 * width), F32),
            jax.ShapeDtypeStruct((3 * width, 2 * width), F32),
            jax.ShapeDtypeStruct((3 * width, 2 * width), F32),
        ),
        in_specs=[
            pl.BlockSpec((3, 1, width, wide), lambda i: (0, i, 0, 0)),
            pl.BlockSpec(small.shape, lambda i: (0, 0, 0)),
        ],
        out_specs=(
            pl.BlockSpec((wide, 3 * width), lambda i: (i, 0)),
            pl.BlockSpec((3 * width, 2 * width), whole),
            pl.BlockSpec((3 * width, 2 * width), whole),
        ),
        compiler_params=pltpu.CompilerParams(vmem_limit_bytes=LIMIT),
        name="finish",
    )(wide_blocks, small)


def solve(rows, cols, covariance, seed_index):
    x = gather(rows, covariance, seed_index)
    wide_blocks, small = main(rows, cols, x, covariance)
    return finish(rows * covariance.shape[0], wide_blocks, small)


def solution(mesh):
    rows, cols = mesh.shape["row"], mesh.shape["col"]
    return jax.shard_map(
        lambda covariance, seed_index: solve(rows, cols, covariance, seed_index),
        mesh=mesh,
        in_specs=(P("row", "col"), P()),
        out_specs=(P("row", None), P(), P()),
        check_vma=False,
    )
```

```python
import functools

import jax
import jax.numpy as jnp
from jax import lax
from jax.experimental import pallas as pl
from jax.experimental.pallas import tpu as pltpu
from jax.sharding import PartitionSpec as P

MESH = pl.DeviceIdType.MESH
F32, BF16 = jnp.float32, jnp.bfloat16
PARTS = 8
AHEAD = 3
LAG = 2
LIMIT = 66 * 1024 * 1024 - 2 * 1024 * 1024

NN = (((1,), (0,)), ((), ()))
NT = (((1,), (1,)), ((), ()))
TN = (((0,), (0,)), ((), ()))


def dot(left, right, dims):
    return lax.dot_general(left, right, dims, precision=lax.Precision.HIGHEST, preferred_element_type=F32)


def halves(value):
    high = value.astype(BF16)
    return high, (value - high.astype(F32)).astype(BF16)


def dot1(left, right, dims):
    return lax.dot_general(left.astype(BF16), right.astype(BF16), dims, preferred_element_type=F32)


def dot3(left, right, dims):
    lh, ll = halves(left)
    rh, rl = halves(right)
    go = functools.partial(lax.dot_general, dimension_numbers=dims, preferred_element_type=F32)
    return go(lh, rh) + (go(lh, rl) + go(ll, rh))


def gather_kernel(rows, index_ref, cov_ref, out_ref, buf, sem):
    width, cols = buf.shape
    wide = cols // rows
    row_count = cov_ref.shape[0]
    base = lax.axis_index("row") * row_count
    tall = lax.broadcasted_iota(jnp.int32, (width, 1), 0)

    def fetch(i, keep):
        place = index_ref[i]
        local = lax.rem(place, row_count)
        pltpu.make_async_copy(cov_ref.at[pl.ds(local, 1), :], buf.at[pl.ds(i, 1), :], sem).start()
        inside = jnp.where(place - local == base, 1, 0)
        return jnp.where(tall == i, inside, keep)

    keep = lax.fori_loop(0, width, fetch, jnp.zeros((width, 1), jnp.int32), unroll=8)
    pltpu.make_async_copy(cov_ref.at[pl.ds(0, width), :], buf, sem).wait()
    for n in range(rows):
        out_ref[n] = jnp.where(keep > 0, buf[:, n * wide : (n + 1) * wide], 0.0)


def gather(rows, covariance, seed_index):
    cols = covariance.shape[1]
    width = seed_index.shape[0]
    return pl.pallas_call(
        functools.partial(gather_kernel, rows),
        out_shape=jax.ShapeDtypeStruct((rows, width, cols // rows), F32),
        in_specs=[pl.BlockSpec(memory_space=pltpu.SMEM), pl.BlockSpec(memory_space=pl.ANY)],
        out_specs=pl.BlockSpec(memory_space=pltpu.VMEM),
        scratch_shapes=[pltpu.VMEM((width, cols), F32), pltpu.SemaphoreType.DMA],
        compiler_params=pltpu.CompilerParams(vmem_limit_bytes=LIMIT),
        name="gather",
    )(seed_index, covariance)


DEEP = 8


def factor_begin(gram, work):
    width = gram.shape[0]
    down = lax.broadcasted_iota(jnp.int32, (width, width), 0)
    across = lax.broadcasted_iota(jnp.int32, (width, width), 1)
    work[:, :width] = gram
    work[:, width:] = jnp.where(down == across, 1.0, 0.0)


def factor_panels(work, begin, end):
    width = work.shape[0]
    deep = DEEP
    across = lax.broadcasted_iota(jnp.int32, (width, width), 1)
    few = lax.broadcasted_iota(jnp.int32, (deep, width), 1)
    tall = lax.broadcasted_iota(jnp.int32, (width, 1), 0)
    short = lax.broadcasted_iota(jnp.int32, (deep, 1), 0)

    def panel(p, carry):
        base = pl.multiple_of(p * deep, deep)
        block = work[pl.ds(base, deep), :]
        now = work[...]
        left, top = now[:, :width], block[:, :width]
        small = [jnp.sum(jnp.where(few == base + t, top, 0.0), axis=1, keepdims=True) for t in range(deep)]
        large = [jnp.sum(jnp.where(across == base + t, left, 0.0), axis=1, keepdims=True) for t in range(deep)]
        for t in range(deep):
            pivot = small[t][t : t + 1]
            scale = lax.rsqrt(pivot)
            scale = scale * (1.5 - 0.5 * pivot * scale * scale)
            unit = block[t : t + 1] * scale
            column = small[t] * scale
            large[t] = large[t] * scale
            for e in range(t + 1, deep):
                factor_e = column[e : e + 1]
                small[e] = small[e] - column * factor_e
                large[e] = large[e] - large[t] * factor_e
            block = jnp.where(short == t, unit, block - jnp.where(short > t, column, 0.0) * unit)
        for t in range(deep):
            now = now - jnp.where(tall >= base + deep, large[t], 0.0) * block[t : t + 1]
        work[...] = now
        work[pl.ds(base, deep), :] = block
        return carry

    lax.fori_loop(begin, end, panel, 0)


def factor_end(work):
    width = work.shape[0]
    down = lax.broadcasted_iota(jnp.int32, (width, width), 0)
    across = lax.broadcasted_iota(jnp.int32, (width, width), 1)
    return jnp.where(down <= across, work[:, :width], 0.0), work[:, width:]


def factor(gram, work):
    factor_begin(gram, work)
    factor_panels(work, 0, work.shape[0] // DEEP)
    return factor_end(work)


def main_kernel(
    rows, cols, root, x_ref, cov_ref,
    wide_ref, tall_ref, small_ref,
    ahi, alo, stage, stage_sem, part, rsbuf, rs_send, rs_recv, st_send, st_recv,
    zbuf, up_send, up_recv, dn_send, dn_recv, rowbuf, pl_send, pl_recv, dd_send, dd_recv, own_sem, out_sem,
    a_loc, a_in, a_z, a_full, a_s1, a_r1, a_s2, a_r2, a_s3, a_r3, work, wsplit, tall,
):
    zs = cols // 2
    width, wide = x_ref.shape[1], x_ref.shape[2]
    row = lax.axis_index("row")
    col = lax.axis_index("col")
    z = col // 2
    core = col % 2
    plane = 2 * rows
    q = row * 2 + core

    deep = stage.shape[1]
    chunks = cov_ref.shape[0] // deep

    def fetch(i):
        return pltpu.make_async_copy(cov_ref.at[pl.ds(i * deep, deep), :], stage.at[i % 2], stage_sem.at[i % 2])

    fetch(0).start()
    barrier = pltpu.get_barrier_semaphore()
    for d in range(1, plane):
        t = lax.rem(q + d, plane)
        pl.semaphore_signal(barrier, inc=1, device_id=(t // 2, 2 * z + t % 2), device_id_type=MESH)
    for d in range(1, zs):
        t = lax.rem(z + d, zs)
        pl.semaphore_signal(barrier, inc=1, device_id=(row, 2 * t + core), device_id_type=MESH)
    pl.semaphore_wait(barrier, plane - 1 + zs - 1)

    pending = []

    def send(src, dst, ssem, rsem, dev):
        return pltpu.make_async_remote_copy(
            src_ref=src, dst_ref=dst, send_sem=ssem, recv_sem=rsem, device_id=dev, device_id_type=MESH
        )

    def rs_copy(u, src, d):
        t = lax.rem(row + d, rows)
        return send(src.at[t], rsbuf.at[u, d - 1], rs_send.at[u, d - 1], rs_recv.at[u, d - 1], (t, col))

    def rs_copies(u, src):
        return [rs_copy(u, src, d) for d in range(1, rows)]

    def rs_start(u, src):
        for copy in rs_copies(u, src):
            copy.start()


    def rs_finish(u, src):
        total = src[row]
        for d, copy in enumerate(rs_copies(u, src)):
            copy.wait_recv()
            total = total + rsbuf[u, d]
        for copy in rs_copies(u, src):
            copy.wait_send()
        return total

    parts = up_send.shape[2]
    thick = width // parts

    def part_of(h):
        return pl.ds(h * thick, thick)

    def up_copy(u, s, h):
        ref = zbuf.at[u, s, part_of(h)]
        return send(ref, ref, up_send.at[u, s, h], up_recv.at[u, s, h], (row, col + 2))

    def dn_copy(u, s, h):
        ref = zbuf.at[u, s, part_of(h)]
        return send(ref, ref, dn_send.at[u, s, h], dn_recv.at[u, s, h], (row, col - 2))

    def slot_of(k, r):
        return k * rows + r

    def plane_copy(u, t, h, d):
        dst = rowbuf.at[u, slot_of(core, row), part_of(h)]
        return send(zbuf.at[u, t, part_of(h)], dst, pl_send.at[u, d, h], pl_recv.at[u, d, h], (t, col))

    def own_copy(u):
        return pltpu.make_async_copy(zbuf.at[u, row], rowbuf.at[u, slot_of(core, row)], own_sem.at[u])

    def to_plane(u, s, h):
        @pl.when(s != row)
        def _():
            plane_copy(u, s, h, lax.rem(s - row + rows, rows)).start()

        if h == parts - 1:
            @pl.when(s == row)
            def _():
                own_copy(u).start()

    def spread_put(u, piece):
        zbuf[u, z] = piece

    def spread_post(u, h):
        @pl.when(z + 1 < zs)
        def _():
            up_copy(u, z, h).start()

        @pl.when(z > 0)
        def _():
            dn_copy(u, z, h).start()

        to_plane(u, z, h)

    ahead = AHEAD

    def spread_step(u, s, h):
        low, high = z - s, z + s

        @pl.when(low >= 0)
        def _():
            up_copy(u, low, h).wait_recv()

            @pl.when(z + 1 < zs)
            def _():
                up_copy(u, low, h).start()

            to_plane(u, low, h)

        @pl.when(high < zs)
        def _():
            dn_copy(u, high, h).wait_recv()

            @pl.when(z > 0)
            def _():
                dn_copy(u, high, h).start()

            to_plane(u, high, h)

    waves = parts + LAG * (zs - 2)

    def spread_wave(u, w):
        for s in reversed(range(1, zs)):
            h = w - LAG * (s - 1)
            if 0 <= h < parts:
                spread_step(u, s, h)

    def spread_steps(u, fillers):
        waiting = list(fillers)
        for w in range(waves):
            while waiting and waiting[0][0] * waves <= w:
                waiting.pop(0)[1]()
            spread_wave(u, w)
            if w + ahead < parts:
                spread_post(u, w + ahead)
        for _, work_of in waiting:
            work_of()

    def partner_copy(u, d, h):
        ref = rowbuf.at[u, slot_of(core, lax.rem(row - d + rows, rows)), part_of(h)]
        return send(ref, ref, dd_send.at[u, d, h], dd_recv.at[u, d, h], (row, col + 1 - 2 * core))

    def spread_half(u):
        own_copy(u).wait()
        for h in range(parts):
            partner_copy(u, 0, h).start()
        for h in range(parts):
            for d in range(1, rows):
                plane_copy(u, row, h, d).wait_recv()
                partner_copy(u, d, h).start()

    def spread_rest(u):
        for h in range(parts):
            for d in range(rows):
                partner_copy(u, d, h).wait_recv()

    def spread_drain(u):
        for h in range(parts):
            for d in range(rows):
                partner_copy(u, d, h).wait_send()
            for d in range(1, rows):
                plane_copy(u, row, h, d).wait_send()
            for s in range(zs):
                @pl.when((z + 1 < zs) & (z >= s))
                def _():
                    up_copy(u, s, h).wait_send()

                @pl.when((z > 0) & (z <= s))
                def _():
                    dn_copy(u, s, h).wait_send()

    def ar_refs(u, m):
        deep = width * m // plane
        return deep, pl.ds(0, deep)

    def ar_one(u, m, d):
        deep, span = ar_refs(u, m)
        t = lax.rem(q + d, plane)
        return send(
            a_loc.at[u, t, span], a_in.at[u, d - 1, span], a_s1.at[u, d - 1], a_r1.at[u, d - 1], (t // 2, 2 * z + t % 2)
        )

    def ar_two(u, m, d):
        deep, span = ar_refs(u, m)
        t = lax.rem(z + d, zs)
        return send(
            a_z.at[u, z, span], a_z.at[u, z, span], a_s2.at[u, d - 1], a_r2.at[u, d - 1], (row, 2 * t + core)
        )

    def ar_three(u, m, d):
        deep, span = ar_refs(u, m)
        t = lax.rem(q + d, plane)
        return send(
            a_full.at[u, q, span], a_full.at[u, q, span], a_s3.at[u, d - 1], a_r3.at[u, d - 1],
            (t // 2, 2 * z + t % 2),
        )

    def ar_start(u, m, value):
        deep, span = ar_refs(u, m)
        for t in range(plane):
            a_loc[u, t, span] = value[t * deep : (t + 1) * deep]
        for d in range(1, plane):
            ar_one(u, m, d).start()

    def ar_mid(u, m):
        deep, span = ar_refs(u, m)
        total = a_loc[u, q, span]
        for d in range(1, plane):
            ar_one(u, m, d).wait_recv()
            total = total + a_in[u, d - 1, span]
        a_z[u, z, span] = total
        for d in range(1, zs):
            ar_two(u, m, d).start()

    def ar_late(u, m):
        deep, span = ar_refs(u, m)
        for d in range(1, zs):
            ar_two(u, m, d).wait_recv()
        total = a_z[u, 0, span]
        for s in range(1, zs):
            total = total + a_z[u, s, span]
        a_full[u, q, span] = total
        for d in range(1, plane):
            ar_three(u, m, d).start()

    def ar_finish(u, m):
        deep, span = ar_refs(u, m)
        for d in range(1, plane):
            ar_three(u, m, d).wait_recv()
        value = jnp.concatenate([a_full[u, t, span] for t in range(plane)], axis=0)
        for d in range(1, plane):
            ar_one(u, m, d).wait_send()
            ar_three(u, m, d).wait_send()
        for d in range(1, zs):
            ar_two(u, m, d).wait_send()
        return value

    def all_sum(u, m, value):
        ar_start(u, m, value)
        ar_mid(u, m)
        ar_late(u, m)
        return ar_finish(u, m)

    def load_covariance(begin, end):
        def chunk(i, carry):
            @pl.when(i + 1 < chunks)
            def _():
                fetch(i + 1).start()

            fetch(i).wait()

            def split(s, inner):
                for n in range(rows):
                    high, low = halves(stage[i % 2, pl.ds(s * 16, 16), n * wide : (n + 1) * wide])
                    ahi[n, pl.ds(i * deep + s * 16, 16), :] = high
                    alo[n, pl.ds(i * deep + s * 16, 16), :] = low
                return inner

            lax.fori_loop(0, deep // 16, split, 0, unroll=4)
            return carry

        lax.fori_loop(begin, end, chunk, 0)

    def half_span(k):
        return pl.ds(pl.multiple_of(k * (rows * wide), rows * wide), rows * wide)

    def split_half(u, k):
        def piece(i, carry):
            j = k * rows + i
            high, low = halves(rowbuf[u, j])
            wsplit[k, :width, pl.ds(pl.multiple_of(i * wide, wide), wide)] = high
            wsplit[k, width:, pl.ds(pl.multiple_of(i * wide, wide), wide)] = low
            return carry

        lax.fori_loop(0, rows, piece, 0)

    def half_term(k, n):
        go = functools.partial(lax.dot_general, dimension_numbers=NN, preferred_element_type=F32)
        one = go(wsplit[k], ahi[n, half_span(k), :])
        two = go(wsplit[k, :width], alo[n, half_span(k), :])
        return one[:width] + one[width:] + two

    early = min(2, rows - 1)

    def product(u, rs):
        split_half(u, core)

        def near(d, carry):
            n = lax.rem(row + d, rows)
            part[n] = half_term(core, n)
            return carry

        lax.fori_loop(1, early + 1, near, 0)
        spread_rest(u)
        split_half(u, 1 - core)

        def far(d, carry):
            n = lax.rem(row + d, rows)
            part[n] = part[n] + half_term(1 - core, n)
            rs_copy(rs, part, d).start()
            return carry

        lax.fori_loop(1, early + 1, far, 0)

        def both(d, carry):
            n = lax.rem(row + d, rows)
            part[n] = half_term(core, n) + half_term(1 - core, n)

            @pl.when(d < rows)
            def _():
                rs_copy(rs, part, d).start()

            return carry

        lax.fori_loop(early + 1, rows + 1, both, 0)

    def scope(name):
        return jax.named_scope(name)

    def rows_to_basis(u, inverse, other, begin, end):
        def piece(j, carry):
            value = rowbuf[u, j]
            if other is not None:
                value = value - dot1(other, rowbuf[0, j], TN)
            value = dot3(inverse, value, NN)
            rowbuf[u, j] = value
            tall[u, pl.ds(pl.multiple_of(j * wide, wide), wide), :] = value.T * root
            return carry

        lax.fori_loop(begin, end, piece, 0)

    def tall_copy(u):
        return pltpu.make_async_copy(tall.at[u], tall_ref.at[u], out_sem.at[u])

    def first_copy(d, h):
        t = lax.rem(row + d, rows)
        return send(
            x_ref.at[t, part_of(h)], rsbuf.at[0, d - 1, part_of(h)], st_send.at[d - 1, h], st_recv.at[d - 1, h], (t, col)
        )

    def first_sum(h):
        span = part_of(h)
        total = x_ref[row, span]
        for d in range(1, rows):
            first_copy(d, h).wait_recv()
            total = total + rsbuf[0, d - 1, span]
        zbuf[0, z, span] = total
        spread_post(0, h)

    def multiply_and_sum(u):
        with scope(f"spread_half#{u}"):
            spread_half(u)
        with scope(f"product#{u}"):
            product(u, u + 1)

    with scope("start#0"):
        for h in range(parts):
            for d in range(1, rows):
                first_copy(d, h).start()
        done = chunks // 4
        load_covariance(0, done)
    with scope("spread_steps#0"):
        for h in range(parts):
            first_sum(h)
            more = chunks // 4 + (chunks - chunks // 4) * (h + 1) // (waves + 1)
            load_covariance(done, more)
            done = more
            if h > 0:
                spread_wave(0, h - 1)
        start = zbuf[0, z]
        ar_start(0, 1, dot(start, start, NT))
        for w in range(parts - 1, waves):
            more = chunks // 4 + (chunks - chunks // 4) * (w + 2) // (waves + 1)
            load_covariance(done, more)
            done = more
            spread_wave(0, w)
        for h in range(parts):
            for d in range(1, rows):
                first_copy(d, h).wait_send()
        ar_mid(0, 1)
    with scope("spread_half#0"):
        spread_half(0)
        ar_late(0, 1)
    with scope("product#0"):
        product(0, 1)
    with scope("factor#0"):
        gram = ar_finish(0, 1)
        upper0, inv0 = factor(gram, work)
        small_ref[0] = upper0
        small_ref[1] = inv0
        q0 = dot(inv0, start, NN)
        spread_drain(0)
    with scope("rs#1"):
        image = rs_finish(1, part)
    with scope("sum#1"):
        image0 = dot(inv0, image, NN)
        ar_start(1, 1, dot(q0, image0, NT))
        rows_to_basis(0, inv0, None, 0, cols // 2)
        ar_mid(1, 1)
        rows_to_basis(0, inv0, None, cols // 2, cols)
        ar_late(1, 1)
        tall_copy(0).start()
        h1 = ar_finish(1, 1)
        once = image0 - dot(h1, q0, TN)
    with scope("spread_start#1"):
        spread_put(1, once)
        for h in range(ahead):
            spread_post(1, h)
        ar_start(2, 2, jnp.concatenate([dot(q0, once, NT), dot(once, once, NT)], axis=0))
    with scope("spread_steps#1"):
        spread_steps(1, [(0.35, lambda: ar_mid(2, 2)), (0.7, lambda: ar_late(2, 2))])
    multiply_and_sum(1)
    with scope("factor#1"):
        both = ar_finish(2, 2)
        h2, raw = both[:width], both[width:]
        gram = raw - dot(h2, h2, TN)
        upper1, inv1 = factor(gram, work)
        small_ref[2] = h1
        small_ref[3] = h2
        small_ref[4] = upper1
        small_ref[5] = inv1
        twice = once - dot(h2, q0, TN)
        q1 = dot(inv1, twice, NN)
        shift = dot(h2, image0, TN)
        stacked = jnp.concatenate([q0, q1], axis=0)
        spread_drain(1)
    with scope("rs#2"):
        image = rs_finish(2, part)
    with scope("sum#3"):
        image1 = dot(inv1, image - shift, NN)
        ar_start(3, 2, dot(stacked, image1, NT))
        rows_to_basis(1, inv1, h2, 0, cols // 2)
        ar_mid(3, 2)
        rows_to_basis(1, inv1, h2, cols // 2, cols)
        ar_late(3, 2)
        tall_copy(1).start()
        g1 = ar_finish(3, 2)
        once = image1 - dot(g1, stacked, TN)
    with scope("last_start#0"):
        spread_put(2, once)
        spread_post(2, 0)
        ar_start(4, 3, jnp.concatenate([dot(stacked, once, NT), dot(once, once, NT)], axis=0))
        for h in range(1, ahead):
            spread_post(2, h)

    def last_gram():
        both = ar_finish(4, 3)
        g2, raw = both[: 2 * width], both[2 * width :]
        small_ref[6] = g1[:width]
        small_ref[7] = g1[width:]
        small_ref[8] = g2[:width]
        small_ref[9] = g2[width:]
        factor_begin(raw - dot(g2, g2, TN), work)

    panels = width // DEEP

    with scope("last_steps#0"):
        spread_steps(2, [
            (0.15, lambda: ar_mid(4, 3)),
            (0.3, lambda: ar_late(4, 3)),
            (0.45, last_gram),
            (0.5, lambda: factor_panels(work, 0, panels // 4)),
            (0.6, lambda: factor_panels(work, panels // 4, panels // 2)),
            (0.7, lambda: factor_panels(work, panels // 2, panels * 3 // 4)),
            (0.8, lambda: factor_panels(work, panels * 3 // 4, panels)),
        ])
    with scope("last_half#0"):
        spread_half(2)
    with scope("factor#2"):
        upper2, inv2 = factor_end(work)
        small_ref[10] = upper2
        small_ref[11] = inv2
    with scope("end#0"):
        spread_rest(2)
        last = pltpu.make_async_copy(rowbuf.at[2], wide_ref, out_sem.at[2])
        last.start()
        spread_drain(2)
        tall_copy(0).wait()
        tall_copy(1).wait()
        last.wait()


def main(rows, cols, x, covariance):
    row_count, col_count = covariance.shape
    width, wide = x.shape[1:]
    zs, plane = cols // 2, 2 * rows
    deep = min(256, row_count)
    dma = pltpu.SemaphoreType.DMA
    uses = 3
    sums, most = 5, 3 * width // plane
    return pl.pallas_call(
        functools.partial(main_kernel, rows, cols, float(rows * row_count) ** 0.5),
        out_shape=(
            jax.ShapeDtypeStruct((cols, width, wide), F32),
            jax.ShapeDtypeStruct((2, row_count, width), F32),
            jax.ShapeDtypeStruct((12, width, width), F32),
        ),
        in_specs=[pl.BlockSpec(memory_space=pltpu.VMEM), pl.BlockSpec(memory_space=pl.ANY)],
        out_specs=(pl.BlockSpec(memory_space=pl.ANY), pl.BlockSpec(memory_space=pl.ANY), pl.BlockSpec(memory_space=pltpu.VMEM)),
        scratch_shapes=[
            pltpu.VMEM((rows, row_count, wide), BF16),
            pltpu.VMEM((rows, row_count, wide), BF16),
            pltpu.VMEM((2, deep, col_count), F32),
            dma((2,)),
            pltpu.VMEM((rows, width, wide), F32),
            pltpu.VMEM((uses, rows - 1, width, wide), F32),
            dma((uses, rows - 1)), dma((uses, rows - 1)), dma((rows - 1, PARTS)), dma((rows - 1, PARTS)),
            pltpu.VMEM((uses, zs, width, wide), F32),
            dma((uses, zs, PARTS)), dma((uses, zs, PARTS)), dma((uses, zs, PARTS)), dma((uses, zs, PARTS)),
            pltpu.VMEM((uses, cols, width, wide), F32),
            dma((uses, rows, PARTS)), dma((uses, rows, PARTS)), dma((uses, rows, PARTS)), dma((uses, rows, PARTS)),
            dma((uses,)), dma((uses,)),
            pltpu.VMEM((sums, plane, most, width), F32),
            pltpu.VMEM((sums, plane - 1, most, width), F32),
            pltpu.VMEM((sums, zs, most, width), F32),
            pltpu.VMEM((sums, plane, most, width), F32),
            dma((sums, plane - 1)), dma((sums, plane - 1)),
            dma((sums, zs - 1)), dma((sums, zs - 1)),
            dma((sums, plane - 1)), dma((sums, plane - 1)),
            pltpu.VMEM((width, 2 * width), F32),
            pltpu.VMEM((2, 2 * width, rows * wide), BF16),
            pltpu.VMEM((2, row_count, width), F32),
        ],
        compiler_params=pltpu.CompilerParams(collective_id=0, has_side_effects=True, vmem_limit_bytes=LIMIT),
        name="lanczos",
    )(x, covariance)


def finish_kernel(root, wide_ref, tall_ref, small_ref, basis_ref, projection_ref, first_ref,
                  wide_buf, tall_buf, out_buf, wide_sem, tall_sem, out_sem):
    width = small_ref.shape[1]
    cols, _, wide = wide_buf.shape

    def get(j):
        rows_of = pl.ds(pl.multiple_of(j * wide, wide), wide)
        return (
            pltpu.make_async_copy(wide_ref.at[j], wide_buf.at[j], wide_sem.at[j]),
            pltpu.make_async_copy(tall_ref.at[:, rows_of], tall_buf.at[:, rows_of], tall_sem.at[j]),
            pltpu.make_async_copy(out_buf.at[rows_of], basis_ref.at[rows_of], out_sem.at[j]),
        )

    for j in range(cols):
        wide_in, tall_in, _ = get(j)
        wide_in.start()
        tall_in.start()
    upper0, inv0, h1, h2, upper1, inv1, g1a, g1b, g2a, g2b, upper2, inv2 = [small_ref[i] for i in range(12)]
    shift = jnp.concatenate([g2a, g2b], axis=0)

    def piece(j, carry):
        wide_in, tall_in, out = get(j)
        wide_in.wait()
        tall_in.wait()
        rows_of = pl.ds(pl.multiple_of(j * wide, wide), wide)
        q0, q1 = tall_buf[0, rows_of], tall_buf[1, rows_of]
        twice = wide_buf[j].T * root - dot1(jnp.concatenate([q0, q1], axis=1), shift, NN)
        out_buf[rows_of, :width] = q0
        out_buf[rows_of, width : 2 * width] = q1
        out_buf[rows_of, 2 * width :] = dot3(twice, inv2, NT)
        out.start()
        return carry

    lax.fori_loop(0, cols, piece, 0)
    zero = jnp.zeros((width, width), F32)
    spot = lambda i: pl.ds(i * width, width)
    for r, c, value in (
        (0, 0, h1 + h2), (1, 0, upper1), (2, 0, zero),
        (0, 1, g1a + g2a), (1, 1, g1b + g2b), (2, 1, upper2),
    ):
        projection_ref[spot(r), spot(c)] = value
    for r, c, value in ((0, 0, h1), (1, 0, zero), (2, 0, zero), (0, 1, g1a), (1, 1, g1b), (2, 1, zero)):
        first_ref[spot(r), spot(c)] = value
    lax.fori_loop(0, cols, lambda j, carry: (get(j)[2].wait(), carry)[1], 0)


def finish(order, wide_block, tall_blocks, small):
    cols, width, wide = wide_block.shape
    dma, vmem, anywhere = pltpu.SemaphoreType.DMA, pl.BlockSpec(memory_space=pltpu.VMEM), pl.BlockSpec(memory_space=pl.ANY)
    return pl.pallas_call(
        functools.partial(finish_kernel, float(order) ** 0.5),
        out_shape=(
            jax.ShapeDtypeStruct((cols * wide, 3 * width), F32),
            jax.ShapeDtypeStruct((3 * width, 2 * width), F32),
            jax.ShapeDtypeStruct((3 * width, 2 * width), F32),
        ),
        in_specs=[anywhere, anywhere, vmem],
        out_specs=(anywhere, vmem, vmem),
        scratch_shapes=[
            pltpu.VMEM(wide_block.shape, F32),
            pltpu.VMEM(tall_blocks.shape, F32),
            pltpu.VMEM((cols * wide, 3 * width), F32),
            dma((cols,)), dma((cols,)), dma((cols,)),
        ],
        compiler_params=pltpu.CompilerParams(vmem_limit_bytes=LIMIT),
        name="finish",
    )(wide_block, tall_blocks, small)


def solve(rows, cols, covariance, seed_index):
    x = gather(rows, covariance, seed_index)
    wide_block, tall_blocks, small = main(rows, cols, x, covariance)
    return finish(rows * covariance.shape[0], wide_block, tall_blocks, small)


def solution(mesh):
    rows, cols = mesh.shape["row"], mesh.shape["col"]
    return jax.shard_map(
        lambda covariance, seed_index: solve(rows, cols, covariance, seed_index),
        mesh=mesh,
        in_specs=(P("row", "col"), P()),
        out_specs=(P("row", None), P(), P()),
        check_vma=False,
    )
```

```python
import functools

import jax
import jax.numpy as jnp
from jax import lax
from jax.experimental import pallas as pl
from jax.experimental.pallas import tpu as pltpu
from jax.sharding import PartitionSpec as P

MESH = pl.DeviceIdType.MESH
F32, BF16 = jnp.float32, jnp.bfloat16
PARTS = 8
AHEAD = 3
LAG = 2
EARLY = 1
LIMIT = 66 * 1024 * 1024 - 2 * 1024 * 1024

NN = (((1,), (0,)), ((), ()))
NT = (((1,), (1,)), ((), ()))
TN = (((0,), (0,)), ((), ()))


def dot(left, right, dims):
    return lax.dot_general(left, right, dims, precision=lax.Precision.HIGHEST, preferred_element_type=F32)


def halves(value):
    high = value.astype(BF16)
    return high, (value - high.astype(F32)).astype(BF16)


def dot1(left, right, dims):
    return lax.dot_general(left.astype(BF16), right.astype(BF16), dims, preferred_element_type=F32)


def dot3(left, right, dims):
    lh, ll = halves(left)
    rh, rl = halves(right)
    go = functools.partial(lax.dot_general, dimension_numbers=dims, preferred_element_type=F32)
    return go(lh, rh) + (go(lh, rl) + go(ll, rh))


def gather_kernel(rows, index_ref, cov_ref, out_ref, buf, sem):
    width, cols = buf.shape
    wide = cols // rows
    row_count = cov_ref.shape[0]
    base = lax.axis_index("row") * row_count
    tall = lax.broadcasted_iota(jnp.int32, (width, 1), 0)

    def fetch(i, keep):
        place = index_ref[i]
        local = place - base
        mine = (local >= 0) & (local < row_count)

        @pl.when(mine)
        def _():
            pltpu.make_async_copy(cov_ref.at[pl.ds(local, 1), :], buf.at[pl.ds(i, 1), :], sem).start()

        return jnp.where(tall == i, jnp.where(mine, 1, 0), keep)

    def drain(i, carry):
        local = index_ref[i] - base

        @pl.when((local >= 0) & (local < row_count))
        def _():
            pltpu.make_async_copy(cov_ref.at[pl.ds(0, 1), :], buf.at[pl.ds(i, 1), :], sem).wait()

        return carry

    keep = lax.fori_loop(0, width, fetch, jnp.zeros((width, 1), jnp.int32), unroll=8)
    lax.fori_loop(0, width, drain, 0, unroll=8)
    for n in range(rows):
        out_ref[n] = jnp.where(keep > 0, buf[:, n * wide : (n + 1) * wide], 0.0)


def gather(rows, covariance, seed_index):
    cols = covariance.shape[1]
    width = seed_index.shape[0]
    return pl.pallas_call(
        functools.partial(gather_kernel, rows),
        out_shape=jax.ShapeDtypeStruct((rows, width, cols // rows), F32),
        in_specs=[pl.BlockSpec(memory_space=pltpu.SMEM), pl.BlockSpec(memory_space=pl.ANY)],
        out_specs=pl.BlockSpec(memory_space=pltpu.VMEM),
        scratch_shapes=[pltpu.VMEM((width, cols), F32), pltpu.SemaphoreType.DMA],
        compiler_params=pltpu.CompilerParams(vmem_limit_bytes=LIMIT),
        name="gather",
    )(seed_index, covariance)


DEEP = 8


def factor_begin(gram, work):
    width = gram.shape[0]
    down = lax.broadcasted_iota(jnp.int32, (width, width), 0)
    across = lax.broadcasted_iota(jnp.int32, (width, width), 1)
    work[:, :width] = gram
    work[:, width:] = jnp.where(down == across, 1.0, 0.0)


def factor_panels(work, begin, end):
    width = work.shape[0]
    deep = DEEP
    across = lax.broadcasted_iota(jnp.int32, (width, width), 1)
    few = lax.broadcasted_iota(jnp.int32, (deep, width), 1)
    tall = lax.broadcasted_iota(jnp.int32, (width, 1), 0)
    short = lax.broadcasted_iota(jnp.int32, (deep, 1), 0)

    def panel(p, carry):
        base = pl.multiple_of(p * deep, deep)
        block = work[pl.ds(base, deep), :]
        now = work[...]
        left, top = now[:, :width], block[:, :width]
        small = [jnp.sum(jnp.where(few == base + t, top, 0.0), axis=1, keepdims=True) for t in range(deep)]
        large = [jnp.sum(jnp.where(across == base + t, left, 0.0), axis=1, keepdims=True) for t in range(deep)]
        for t in range(deep):
            pivot = small[t][t : t + 1]
            scale = lax.rsqrt(pivot)
            scale = scale * (1.5 - 0.5 * pivot * scale * scale)
            unit = block[t : t + 1] * scale
            column = small[t] * scale
            large[t] = large[t] * scale
            for e in range(t + 1, deep):
                factor_e = column[e : e + 1]
                small[e] = small[e] - column * factor_e
                large[e] = large[e] - large[t] * factor_e
            block = jnp.where(short == t, unit, block - jnp.where(short > t, column, 0.0) * unit)
        for t in range(deep):
            now = now - jnp.where(tall >= base + deep, large[t], 0.0) * block[t : t + 1]
        work[...] = now
        work[pl.ds(base, deep), :] = block
        return carry

    lax.fori_loop(begin, end, panel, 0)


def factor_end(work):
    width = work.shape[0]
    down = lax.broadcasted_iota(jnp.int32, (width, width), 0)
    across = lax.broadcasted_iota(jnp.int32, (width, width), 1)
    return jnp.where(down <= across, work[:, :width], 0.0), work[:, width:]


def factor(gram, work):
    factor_begin(gram, work)
    factor_panels(work, 0, work.shape[0] // DEEP)
    return factor_end(work)


def main_kernel(
    rows, cols, root, x_ref, cov_ref,
    wide_ref, tall_ref, small_ref,
    ahi, alo, stage, stage_sem, part, rsbuf, rs_send, rs_recv, st_send, st_recv,
    zbuf, up_send, up_recv, dn_send, dn_recv, rowbuf, pl_send, pl_recv, dd_send, dd_recv, own_sem, out_sem,
    a_loc, a_in, a_z, a_full, a_s1, a_r1, a_s2, a_r2, a_s3, a_r3, work, wsplit, tall,
):
    zs = cols // 2
    width, wide = x_ref.shape[1], x_ref.shape[2]
    row = lax.axis_index("row")
    col = lax.axis_index("col")
    z = col // 2
    core = col % 2
    plane = 2 * rows
    q = row * 2 + core

    deep = stage.shape[1]
    chunks = cov_ref.shape[0] // deep

    def fetch(i):
        return pltpu.make_async_copy(cov_ref.at[pl.ds(i * deep, deep), :], stage.at[i % 2], stage_sem.at[i % 2])

    fetch(0).start()
    barrier = pltpu.get_barrier_semaphore()
    for d in range(1, plane):
        t = lax.rem(q + d, plane)
        pl.semaphore_signal(barrier, inc=1, device_id=(t // 2, 2 * z + t % 2), device_id_type=MESH)
    for d in range(1, zs):
        t = lax.rem(z + d, zs)
        pl.semaphore_signal(barrier, inc=1, device_id=(row, 2 * t + core), device_id_type=MESH)
    pl.semaphore_wait(barrier, plane - 1 + zs - 1)

    pending = []

    def send(src, dst, ssem, rsem, dev):
        return pltpu.make_async_remote_copy(
            src_ref=src, dst_ref=dst, send_sem=ssem, recv_sem=rsem, device_id=dev, device_id_type=MESH
        )

    def rs_copy(u, src, d):
        t = lax.rem(row + d, rows)
        return send(src.at[t], rsbuf.at[u, d - 1], rs_send.at[u, d - 1], rs_recv.at[u, d - 1], (t, col))

    def rs_copies(u, src):
        return [rs_copy(u, src, d) for d in range(1, rows)]

    def rs_start(u, src):
        for copy in rs_copies(u, src):
            copy.start()


    def rs_finish(u, src):
        total = src[row]
        for d, copy in enumerate(rs_copies(u, src)):
            copy.wait_recv()
            total = total + rsbuf[u, d]
        for copy in rs_copies(u, src):
            copy.wait_send()
        return total

    parts = up_send.shape[2]
    thick = width // parts

    def part_of(h):
        return pl.ds(h * thick, thick)

    def up_copy(u, s, h):
        ref = zbuf.at[u, s, part_of(h)]
        return send(ref, ref, up_send.at[u, s, h], up_recv.at[u, s, h], (row, col + 2))

    def dn_copy(u, s, h):
        ref = zbuf.at[u, s, part_of(h)]
        return send(ref, ref, dn_send.at[u, s, h], dn_recv.at[u, s, h], (row, col - 2))

    def slot_of(k, r):
        return k * rows + r

    def plane_copy(u, t, h, d):
        dst = rowbuf.at[u, slot_of(core, row), part_of(h)]
        return send(zbuf.at[u, t, part_of(h)], dst, pl_send.at[u, d, h], pl_recv.at[u, d, h], (t, col))

    def own_copy(u):
        return pltpu.make_async_copy(zbuf.at[u, row], rowbuf.at[u, slot_of(core, row)], own_sem.at[u])

    def to_plane(u, s, h):
        @pl.when(s != row)
        def _():
            plane_copy(u, s, h, lax.rem(s - row + rows, rows)).start()

        if h == parts - 1:
            @pl.when(s == row)
            def _():
                own_copy(u).start()

    def spread_put(u, piece):
        zbuf[u, z] = piece

    def spread_post(u, h):
        @pl.when(z + 1 < zs)
        def _():
            up_copy(u, z, h).start()

        @pl.when(z > 0)
        def _():
            dn_copy(u, z, h).start()

        to_plane(u, z, h)

    ahead = AHEAD

    def spread_step(u, s, h):
        low, high = z - s, z + s

        @pl.when(low >= 0)
        def _():
            up_copy(u, low, h).wait_recv()

            @pl.when(z + 1 < zs)
            def _():
                up_copy(u, low, h).start()

            to_plane(u, low, h)

        @pl.when(high < zs)
        def _():
            dn_copy(u, high, h).wait_recv()

            @pl.when(z > 0)
            def _():
                dn_copy(u, high, h).start()

            to_plane(u, high, h)

    waves = parts + LAG * (zs - 2)

    def spread_wave(u, w):
        for s in reversed(range(1, zs)):
            h = w - LAG * (s - 1)
            if 0 <= h < parts:
                spread_step(u, s, h)

    def spread_steps(u, fillers):
        waiting = list(fillers)
        for w in range(waves):
            while waiting and waiting[0][0] * waves <= w:
                waiting.pop(0)[1]()
            spread_wave(u, w)
            if w + ahead < parts:
                spread_post(u, w + ahead)
        for _, work_of in waiting:
            work_of()

    def partner_copy(u, d, h):
        ref = rowbuf.at[u, slot_of(core, lax.rem(row - d + rows, rows)), part_of(h)]
        return send(ref, ref, dd_send.at[u, d, h], dd_recv.at[u, d, h], (row, col + 1 - 2 * core))

    def spread_half(u):
        own_copy(u).wait()
        for h in range(parts):
            partner_copy(u, 0, h).start()
        for h in range(parts):
            for d in range(1, rows):
                plane_copy(u, row, h, d).wait_recv()
                partner_copy(u, d, h).start()

    def spread_rest(u):
        for h in range(parts):
            for d in range(rows):
                partner_copy(u, d, h).wait_recv()

    def spread_drain(u):
        for h in range(parts):
            for d in range(rows):
                partner_copy(u, d, h).wait_send()
            for d in range(1, rows):
                plane_copy(u, row, h, d).wait_send()
            for s in range(zs):
                @pl.when((z + 1 < zs) & (z >= s))
                def _():
                    up_copy(u, s, h).wait_send()

                @pl.when((z > 0) & (z <= s))
                def _():
                    dn_copy(u, s, h).wait_send()

    def ar_refs(u, m):
        deep = width * m // plane
        return deep, pl.ds(0, deep)

    def ar_one(u, m, d):
        deep, span = ar_refs(u, m)
        t = lax.rem(q + d, plane)
        return send(
            a_loc.at[u, t, span], a_in.at[u, d - 1, span], a_s1.at[u, d - 1], a_r1.at[u, d - 1], (t // 2, 2 * z + t % 2)
        )

    def ar_two(u, m, d):
        deep, span = ar_refs(u, m)
        t = lax.rem(z + d, zs)
        return send(
            a_z.at[u, z, span], a_z.at[u, z, span], a_s2.at[u, d - 1], a_r2.at[u, d - 1], (row, 2 * t + core)
        )

    def ar_three(u, m, d):
        deep, span = ar_refs(u, m)
        t = lax.rem(q + d, plane)
        return send(
            a_full.at[u, q, span], a_full.at[u, q, span], a_s3.at[u, d - 1], a_r3.at[u, d - 1],
            (t // 2, 2 * z + t % 2),
        )

    def ar_start(u, m, value):
        deep, span = ar_refs(u, m)
        for t in range(plane):
            a_loc[u, t, span] = value[t * deep : (t + 1) * deep]
        for d in range(1, plane):
            ar_one(u, m, d).start()

    def ar_mid(u, m):
        deep, span = ar_refs(u, m)
        total = a_loc[u, q, span]
        for d in range(1, plane):
            ar_one(u, m, d).wait_recv()
            total = total + a_in[u, d - 1, span]
        a_z[u, z, span] = total
        for d in range(1, zs):
            ar_two(u, m, d).start()

    def ar_late(u, m):
        deep, span = ar_refs(u, m)
        for d in range(1, zs):
            ar_two(u, m, d).wait_recv()
        total = a_z[u, 0, span]
        for s in range(1, zs):
            total = total + a_z[u, s, span]
        a_full[u, q, span] = total
        for d in range(1, plane):
            ar_three(u, m, d).start()

    def ar_finish(u, m):
        deep, span = ar_refs(u, m)
        for d in range(1, plane):
            ar_three(u, m, d).wait_recv()
        value = jnp.concatenate([a_full[u, t, span] for t in range(plane)], axis=0)
        for d in range(1, plane):
            ar_one(u, m, d).wait_send()
            ar_three(u, m, d).wait_send()
        for d in range(1, zs):
            ar_two(u, m, d).wait_send()
        return value

    def all_sum(u, m, value):
        ar_start(u, m, value)
        ar_mid(u, m)
        ar_late(u, m)
        return ar_finish(u, m)

    def load_covariance(begin, end):
        def chunk(i, carry):
            @pl.when(i + 1 < chunks)
            def _():
                fetch(i + 1).start()

            fetch(i).wait()

            def split(s, inner):
                for n in range(rows):
                    high, low = halves(stage[i % 2, pl.ds(s * 16, 16), n * wide : (n + 1) * wide])
                    ahi[n, pl.ds(i * deep + s * 16, 16), :] = high
                    alo[n, pl.ds(i * deep + s * 16, 16), :] = low
                return inner

            lax.fori_loop(0, deep // 16, split, 0, unroll=4)
            return carry

        lax.fori_loop(begin, end, chunk, 0)

    def half_span(k):
        return pl.ds(pl.multiple_of(k * (rows * wide), rows * wide), rows * wide)

    def split_half(u, k):
        def piece(i, carry):
            j = k * rows + i
            high, low = halves(rowbuf[u, j])
            wsplit[k, :width, pl.ds(pl.multiple_of(i * wide, wide), wide)] = high
            wsplit[k, width:, pl.ds(pl.multiple_of(i * wide, wide), wide)] = low
            return carry

        lax.fori_loop(0, rows, piece, 0)

    def half_term(k, n):
        go = functools.partial(lax.dot_general, dimension_numbers=NN, preferred_element_type=F32)
        one = go(wsplit[k], ahi[n, half_span(k), :])
        two = go(wsplit[k, :width], alo[n, half_span(k), :])
        return one[:width] + one[width:] + two

    early = min(EARLY, rows - 1)

    def product(u, rs):
        split_half(u, core)

        def near(d, carry):
            n = lax.rem(row + d, rows)
            part[n] = half_term(core, n)
            return carry

        lax.fori_loop(1, early + 1, near, 0)
        spread_rest(u)
        split_half(u, 1 - core)

        def far(d, carry):
            n = lax.rem(row + d, rows)
            part[n] = part[n] + half_term(1 - core, n)
            rs_copy(rs, part, d).start()
            return carry

        lax.fori_loop(1, early + 1, far, 0)

        def both(d, carry):
            n = lax.rem(row + d, rows)
            part[n] = half_term(core, n) + half_term(1 - core, n)

            @pl.when(d < rows)
            def _():
                rs_copy(rs, part, d).start()

            return carry

        lax.fori_loop(early + 1, rows + 1, both, 0)

    def scope(name):
        return jax.named_scope(name)

    def rows_to_basis(u, inverse, other, begin, end):
        def piece(j, carry):
            value = rowbuf[u, j]
            if other is not None:
                value = value - dot1(other, rowbuf[0, j], TN)
            value = dot3(inverse, value, NN)
            rowbuf[u, j] = value
            tall[u, pl.ds(pl.multiple_of(j * wide, wide), wide), :] = value.T * root
            return carry

        lax.fori_loop(begin, end, piece, 0)

    def tall_copy(u):
        return pltpu.make_async_copy(tall.at[u], tall_ref.at[u], out_sem.at[u])

    def first_copy(d, h):
        t = lax.rem(row + d, rows)
        return send(
            x_ref.at[t, part_of(h)], rsbuf.at[0, d - 1, part_of(h)], st_send.at[d - 1, h], st_recv.at[d - 1, h], (t, col)
        )

    def first_sum(h):
        span = part_of(h)
        total = x_ref[row, span]
        for d in range(1, rows):
            first_copy(d, h).wait_recv()
            total = total + rsbuf[0, d - 1, span]
        zbuf[0, z, span] = total
        spread_post(0, h)

    def multiply_and_sum(u):
        with scope(f"spread_half#{u}"):
            spread_half(u)
        with scope(f"product#{u}"):
            product(u, u + 1)

    with scope("start#0"):
        for h in range(parts):
            for d in range(1, rows):
                first_copy(d, h).start()
        done = chunks // 4
        load_covariance(0, done)
    with scope("spread_steps#0"):
        for h in range(parts):
            first_sum(h)
            more = chunks // 4 + (chunks - chunks // 4) * (h + 1) // (waves + 1)
            load_covariance(done, more)
            done = more
            if h > 0:
                spread_wave(0, h - 1)
        start = zbuf[0, z]
        ar_start(0, 1, dot(start, start, NT))
        for w in range(parts - 1, waves):
            more = chunks // 4 + (chunks - chunks // 4) * (w + 2) // (waves + 1)
            load_covariance(done, more)
            done = more
            spread_wave(0, w)
        for h in range(parts):
            for d in range(1, rows):
                first_copy(d, h).wait_send()
        ar_mid(0, 1)
    with scope("spread_half#0"):
        spread_half(0)
        ar_late(0, 1)
    with scope("product#0"):
        product(0, 1)
    with scope("factor#0"):
        gram = ar_finish(0, 1)
        upper0, inv0 = factor(gram, work)
        small_ref[0] = upper0
        small_ref[1] = inv0
        q0 = dot(inv0, start, NN)
        spread_drain(0)
    with scope("rs#1"):
        image = rs_finish(1, part)
    with scope("sum#1"):
        image0 = dot(inv0, image, NN)
        ar_start(1, 1, dot(q0, image0, NT))
        rows_to_basis(0, inv0, None, 0, cols // 2)
        ar_mid(1, 1)
        rows_to_basis(0, inv0, None, cols // 2, cols)
        ar_late(1, 1)
        tall_copy(0).start()
        h1 = ar_finish(1, 1)
        once = image0 - dot(h1, q0, TN)
    with scope("spread_start#1"):
        spread_put(1, once)
        for h in range(ahead):
            spread_post(1, h)
        ar_start(2, 2, jnp.concatenate([dot(q0, once, NT), dot(once, once, NT)], axis=0))

    panels = width // DEEP
    kept = {}

    def second_gram():
        both = ar_finish(2, 2)
        h2, raw = both[:width], both[width:]
        factor_begin(raw - dot(h2, h2, TN), work)
        small_ref[2] = h1
        small_ref[3] = h2
        kept["h2"] = h2

    def second_factor():
        h2 = kept["h2"]
        upper1, inv1 = factor_end(work)
        small_ref[4] = upper1
        small_ref[5] = inv1
        twice = once - dot(h2, q0, TN)
        kept["inv1"] = inv1
        kept["stacked"] = jnp.concatenate([q0, dot(inv1, twice, NN)], axis=0)
        kept["shift"] = dot(h2, image0, TN)

    with scope("spread_steps#1"):
        spread_steps(1, [
            (0.35, lambda: ar_mid(2, 2)), (0.7, lambda: ar_late(2, 2)),
        ])
    multiply_and_sum(1)
    with scope("factor#1"):
        second_gram()
        factor_panels(work, 0, panels)
        second_factor()
        spread_drain(1)
        h2, inv1, stacked = kept["h2"], kept["inv1"], kept["stacked"]
    with scope("rs#2"):
        image = rs_finish(2, part)
    with scope("last_start#0"):
        image1 = dot(inv1, image - kept["shift"], NN)
        spread_put(2, image1)
        spread_post(2, 0)
        ar_start(3, 2, dot(stacked, image1, NT))
        for h in range(1, ahead):
            spread_post(2, h)

    def basis_part(i):
        return lambda: rows_to_basis(1, inv1, h2, cols * i // 4, cols * (i + 1) // 4)

    def last_project():
        g1 = ar_finish(3, 2)
        once = image1 - dot(g1, stacked, TN)
        ar_start(4, 3, jnp.concatenate([dot(stacked, once, NT), dot(once, once, NT)], axis=0))
        small_ref[6] = g1[:width]
        small_ref[7] = g1[width:]
        kept["g1"] = g1

    def fold_spot(j, b):
        return pl.ds(pl.multiple_of(j * wide + b * width, width), width)

    def fold_part(i):
        def piece(j, carry):
            value = dot3(kept["g1"], jnp.concatenate([rowbuf[0, j], rowbuf[1, j]], axis=0), TN)
            for b in range(wide // width):
                tall[0, fold_spot(j, b), :] = value[:, b * width : (b + 1) * width]
            return carry

        return lambda: lax.fori_loop(cols * i // 4, cols * (i + 1) // 4, piece, 0)

    def fold():
        def piece(j, carry):
            for b in range(wide // width):
                span = slice(b * width, (b + 1) * width)
                rowbuf[2, j, :, span] = rowbuf[2, j, :, span] - tall[0, fold_spot(j, b), :]
            return carry

        lax.fori_loop(0, cols, piece, 0)

    def last_gram():
        both = ar_finish(4, 3)
        g2, raw = both[: 2 * width], both[2 * width :]
        small_ref[8] = g2[:width]
        small_ref[9] = g2[width:]
        factor_begin(raw - dot(g2, g2, TN), work)

    with scope("last_steps#0"):
        spread_steps(2, [
            (0.0, basis_part(0)), (0.1, lambda: ar_mid(3, 2)), (0.1, basis_part(1)), (0.25, lambda: ar_late(3, 2)),
            (0.25, basis_part(2)), (0.4, last_project), (0.4, basis_part(3)), (0.4, lambda: tall_copy(1).start()),
            (0.5, lambda: tall_copy(0).wait()), (0.5, fold_part(0)),
            (0.6, lambda: ar_mid(4, 3)), (0.6, fold_part(1)), (0.7, fold_part(2)), (0.8, lambda: ar_late(4, 3)),
            (0.85, fold_part(3)),
        ])
    with scope("last_gram#0"):
        last_gram()
        factor_panels(work, 0, panels // 2)
    with scope("last_half#0"):
        spread_half(2)
    with scope("factor#2"):
        factor_panels(work, panels // 2, panels)
        upper2, inv2 = factor_end(work)
        small_ref[10] = upper2
        small_ref[11] = inv2
    with scope("end#0"):
        spread_rest(2)
        spread_drain(2)
        fold()
        last = pltpu.make_async_copy(rowbuf.at[2], wide_ref, out_sem.at[2])
        last.start()
        tall_copy(1).wait()
        last.wait()


def main(rows, cols, x, covariance):
    row_count, col_count = covariance.shape
    width, wide = x.shape[1:]
    zs, plane = cols // 2, 2 * rows
    deep = min(256, row_count)
    dma = pltpu.SemaphoreType.DMA
    uses = 3
    sums, most = 5, 3 * width // plane
    return pl.pallas_call(
        functools.partial(main_kernel, rows, cols, float(rows * row_count) ** 0.5),
        out_shape=(
            jax.ShapeDtypeStruct((cols, width, wide), F32),
            jax.ShapeDtypeStruct((2, row_count, width), F32),
            jax.ShapeDtypeStruct((12, width, width), F32),
        ),
        in_specs=[pl.BlockSpec(memory_space=pltpu.VMEM), pl.BlockSpec(memory_space=pl.ANY)],
        out_specs=(pl.BlockSpec(memory_space=pl.ANY), pl.BlockSpec(memory_space=pl.ANY), pl.BlockSpec(memory_space=pltpu.VMEM)),
        scratch_shapes=[
            pltpu.VMEM((rows, row_count, wide), BF16),
            pltpu.VMEM((rows, row_count, wide), BF16),
            pltpu.VMEM((2, deep, col_count), F32),
            dma((2,)),
            pltpu.VMEM((rows, width, wide), F32),
            pltpu.VMEM((uses, rows - 1, width, wide), F32),
            dma((uses, rows - 1)), dma((uses, rows - 1)), dma((rows - 1, PARTS)), dma((rows - 1, PARTS)),
            pltpu.VMEM((uses, zs, width, wide), F32),
            dma((uses, zs, PARTS)), dma((uses, zs, PARTS)), dma((uses, zs, PARTS)), dma((uses, zs, PARTS)),
            pltpu.VMEM((uses, cols, width, wide), F32),
            dma((uses, rows, PARTS)), dma((uses, rows, PARTS)), dma((uses, rows, PARTS)), dma((uses, rows, PARTS)),
            dma((uses,)), dma((uses,)),
            pltpu.VMEM((sums, plane, most, width), F32),
            pltpu.VMEM((sums, plane - 1, most, width), F32),
            pltpu.VMEM((sums, zs, most, width), F32),
            pltpu.VMEM((sums, plane, most, width), F32),
            dma((sums, plane - 1)), dma((sums, plane - 1)),
            dma((sums, zs - 1)), dma((sums, zs - 1)),
            dma((sums, plane - 1)), dma((sums, plane - 1)),
            pltpu.VMEM((width, 2 * width), F32),
            pltpu.VMEM((2, 2 * width, rows * wide), BF16),
            pltpu.VMEM((2, row_count, width), F32),
        ],
        compiler_params=pltpu.CompilerParams(collective_id=0, has_side_effects=True, vmem_limit_bytes=LIMIT),
        name="lanczos",
    )(x, covariance)


def finish_kernel(root, wide_ref, tall_ref, small_ref, basis_ref, projection_ref, first_ref,
                  wide_buf, tall_buf, out_buf, wide_sem, tall_sem, out_sem):
    width = small_ref.shape[1]
    cols, _, wide = wide_buf.shape

    def get(j):
        rows_of = pl.ds(pl.multiple_of(j * wide, wide), wide)
        return (
            pltpu.make_async_copy(wide_ref.at[j], wide_buf.at[j], wide_sem.at[j]),
            pltpu.make_async_copy(tall_ref.at[:, rows_of], tall_buf.at[:, rows_of], tall_sem.at[j]),
            pltpu.make_async_copy(out_buf.at[rows_of], basis_ref.at[rows_of], out_sem.at[j]),
        )

    for j in range(cols):
        wide_in, tall_in, _ = get(j)
        wide_in.start()
        tall_in.start()
    upper0, inv0, h1, h2, upper1, inv1, g1a, g1b, g2a, g2b, upper2, inv2 = [small_ref[i] for i in range(12)]
    shift = jnp.concatenate([g2a, g2b], axis=0)

    def piece(j, carry):
        wide_in, tall_in, out = get(j)
        wide_in.wait()
        tall_in.wait()
        rows_of = pl.ds(pl.multiple_of(j * wide, wide), wide)
        q0, q1 = tall_buf[0, rows_of], tall_buf[1, rows_of]
        twice = wide_buf[j].T * root - dot1(jnp.concatenate([q0, q1], axis=1), shift, NN)
        out_buf[rows_of, :width] = q0
        out_buf[rows_of, width : 2 * width] = q1
        out_buf[rows_of, 2 * width :] = dot3(twice, inv2, NT)
        out.start()
        return carry

    lax.fori_loop(0, cols, piece, 0)
    zero = jnp.zeros((width, width), F32)
    spot = lambda i: pl.ds(i * width, width)
    for r, c, value in (
        (0, 0, h1 + h2), (1, 0, upper1), (2, 0, zero),
        (0, 1, g1a + g2a), (1, 1, g1b + g2b), (2, 1, upper2),
    ):
        projection_ref[spot(r), spot(c)] = value
    for r, c, value in ((0, 0, h1), (1, 0, zero), (2, 0, zero), (0, 1, g1a), (1, 1, g1b), (2, 1, zero)):
        first_ref[spot(r), spot(c)] = value
    lax.fori_loop(0, cols, lambda j, carry: (get(j)[2].wait(), carry)[1], 0)


def finish(order, wide_block, tall_blocks, small):
    cols, width, wide = wide_block.shape
    dma, vmem, anywhere = pltpu.SemaphoreType.DMA, pl.BlockSpec(memory_space=pltpu.VMEM), pl.BlockSpec(memory_space=pl.ANY)
    return pl.pallas_call(
        functools.partial(finish_kernel, float(order) ** 0.5),
        out_shape=(
            jax.ShapeDtypeStruct((cols * wide, 3 * width), F32),
            jax.ShapeDtypeStruct((3 * width, 2 * width), F32),
            jax.ShapeDtypeStruct((3 * width, 2 * width), F32),
        ),
        in_specs=[anywhere, anywhere, vmem],
        out_specs=(anywhere, vmem, vmem),
        scratch_shapes=[
            pltpu.VMEM(wide_block.shape, F32),
            pltpu.VMEM(tall_blocks.shape, F32),
            pltpu.VMEM((cols * wide, 3 * width), F32),
            dma((cols,)), dma((cols,)), dma((cols,)),
        ],
        compiler_params=pltpu.CompilerParams(vmem_limit_bytes=LIMIT),
        name="finish",
    )(wide_block, tall_blocks, small)


def solve(rows, cols, covariance, seed_index):
    x = gather(rows, covariance, seed_index)
    wide_block, tall_blocks, small = main(rows, cols, x, covariance)
    return finish(rows * covariance.shape[0], wide_block, tall_blocks, small)


def solution(mesh):
    rows, cols = mesh.shape["row"], mesh.shape["col"]
    return jax.shard_map(
        lambda covariance, seed_index: solve(rows, cols, covariance, seed_index),
        mesh=mesh,
        in_specs=(P("row", "col"), P()),
        out_specs=(P("row", None), P(), P()),
        check_vma=False,
    )
```

```python
import functools

import jax
import jax.numpy as jnp
from jax import lax
from jax.experimental import pallas as pl
from jax.experimental.pallas import tpu as pltpu
from jax.sharding import PartitionSpec as P

MESH = pl.DeviceIdType.MESH
F32, BF16 = jnp.float32, jnp.bfloat16
PARTS = 8
AHEAD = 3
LAG = 2
EARLY = 1
LIMIT = 66 * 1024 * 1024 - 2 * 1024 * 1024

NN = (((1,), (0,)), ((), ()))
NT = (((1,), (1,)), ((), ()))
TN = (((0,), (0,)), ((), ()))


def dot(left, right, dims):
    return lax.dot_general(left, right, dims, precision=lax.Precision.HIGHEST, preferred_element_type=F32)


def halves(value):
    high = value.astype(BF16)
    return high, (value - high.astype(F32)).astype(BF16)


def dot1(left, right, dims):
    return lax.dot_general(left.astype(BF16), right.astype(BF16), dims, preferred_element_type=F32)


def dot3(left, right, dims):
    lh, ll = halves(left)
    rh, rl = halves(right)
    go = functools.partial(lax.dot_general, dimension_numbers=dims, preferred_element_type=F32)
    return go(lh, rh) + (go(lh, rl) + go(ll, rh))


def gather_kernel(rows, index_ref, cov_ref, out_ref, buf, sem):
    width, cols = buf.shape
    wide = cols // rows
    row_count = cov_ref.shape[0]
    base = lax.axis_index("row") * row_count
    tall = lax.broadcasted_iota(jnp.int32, (width, 1), 0)

    def fetch(i, keep):
        place = index_ref[i]
        local = place - base
        mine = (local >= 0) & (local < row_count)

        @pl.when(mine)
        def _():
            pltpu.make_async_copy(cov_ref.at[pl.ds(local, 1), :], buf.at[pl.ds(i, 1), :], sem).start()

        return jnp.where(tall == i, jnp.where(mine, 1, 0), keep)

    def drain(i, carry):
        local = index_ref[i] - base

        @pl.when((local >= 0) & (local < row_count))
        def _():
            pltpu.make_async_copy(cov_ref.at[pl.ds(0, 1), :], buf.at[pl.ds(i, 1), :], sem).wait()

        return carry

    keep = lax.fori_loop(0, width, fetch, jnp.zeros((width, 1), jnp.int32), unroll=8)
    lax.fori_loop(0, width, drain, 0, unroll=8)
    for n in range(rows):
        out_ref[n] = jnp.where(keep > 0, buf[:, n * wide : (n + 1) * wide], 0.0)


def gather(rows, covariance, seed_index):
    cols = covariance.shape[1]
    width = seed_index.shape[0]
    return pl.pallas_call(
        functools.partial(gather_kernel, rows),
        out_shape=jax.ShapeDtypeStruct((rows, width, cols // rows), F32),
        in_specs=[pl.BlockSpec(memory_space=pltpu.SMEM), pl.BlockSpec(memory_space=pl.ANY)],
        out_specs=pl.BlockSpec(memory_space=pltpu.VMEM),
        scratch_shapes=[pltpu.VMEM((width, cols), F32), pltpu.SemaphoreType.DMA],
        compiler_params=pltpu.CompilerParams(vmem_limit_bytes=LIMIT),
        name="gather",
    )(seed_index, covariance)


DEEP = 8


def factor_begin(gram, work):
    width = gram.shape[0]
    down = lax.broadcasted_iota(jnp.int32, (width, width), 0)
    across = lax.broadcasted_iota(jnp.int32, (width, width), 1)
    work[:, :width] = gram
    work[:, width:] = jnp.where(down == across, 1.0, 0.0)


def factor_panels(work, begin, end):
    width = work.shape[0]
    deep = DEEP
    across = lax.broadcasted_iota(jnp.int32, (width, width), 1)
    few = lax.broadcasted_iota(jnp.int32, (deep, width), 1)
    tall = lax.broadcasted_iota(jnp.int32, (width, 1), 0)
    short = lax.broadcasted_iota(jnp.int32, (deep, 1), 0)

    def panel(p, carry):
        base = pl.multiple_of(p * deep, deep)
        block = work[pl.ds(base, deep), :]
        now = work[...]
        left, top = now[:, :width], block[:, :width]
        small = [jnp.sum(jnp.where(few == base + t, top, 0.0), axis=1, keepdims=True) for t in range(deep)]
        large = [jnp.sum(jnp.where(across == base + t, left, 0.0), axis=1, keepdims=True) for t in range(deep)]
        for t in range(deep):
            pivot = small[t][t : t + 1]
            scale = lax.rsqrt(pivot)
            scale = scale * (1.5 - 0.5 * pivot * scale * scale)
            unit = block[t : t + 1] * scale
            column = small[t] * scale
            large[t] = large[t] * scale
            for e in range(t + 1, deep):
                factor_e = column[e : e + 1]
                small[e] = small[e] - column * factor_e
                large[e] = large[e] - large[t] * factor_e
            block = jnp.where(short == t, unit, block - jnp.where(short > t, column, 0.0) * unit)
        for t in range(deep):
            now = now - jnp.where(tall >= base + deep, large[t], 0.0) * block[t : t + 1]
        work[...] = now
        work[pl.ds(base, deep), :] = block
        return carry

    lax.fori_loop(begin, end, panel, 0)


def factor_end(work):
    width = work.shape[0]
    down = lax.broadcasted_iota(jnp.int32, (width, width), 0)
    across = lax.broadcasted_iota(jnp.int32, (width, width), 1)
    return jnp.where(down <= across, work[:, :width], 0.0), work[:, width:]


def factor(gram, work):
    factor_begin(gram, work)
    factor_panels(work, 0, work.shape[0] // DEEP)
    return factor_end(work)


def main_kernel(
    rows, cols, root, x_ref, cov_ref,
    wide_ref, tall_ref, small_ref,
    ahi, alo, stage, stage_sem, part, rsbuf, rs_send, rs_recv, st_send, st_recv,
    zbuf, up_send, up_recv, dn_send, dn_recv, rowbuf, pl_send, pl_recv, dd_send, dd_recv, own_sem, out_sem,
    a_loc, a_in, a_z, a_full, a_s1, a_r1, a_s2, a_r2, a_s3, a_r3, work, wsplit, tall,
):
    zs = cols // 2
    width, wide = x_ref.shape[1], x_ref.shape[2]
    row = lax.axis_index("row")
    col = lax.axis_index("col")
    z = col // 2
    core = col % 2
    plane = 2 * rows
    q = row * 2 + core

    deep = stage.shape[1]
    chunks = cov_ref.shape[0] // deep

    def fetch(i):
        return pltpu.make_async_copy(cov_ref.at[pl.ds(i * deep, deep), :], stage.at[i % 2], stage_sem.at[i % 2])

    fetch(0).start()
    barrier = pltpu.get_barrier_semaphore()
    for d in range(1, plane):
        t = lax.rem(q + d, plane)
        pl.semaphore_signal(barrier, inc=1, device_id=(t // 2, 2 * z + t % 2), device_id_type=MESH)
    for d in range(1, zs):
        t = lax.rem(z + d, zs)
        pl.semaphore_signal(barrier, inc=1, device_id=(row, 2 * t + core), device_id_type=MESH)
    pl.semaphore_wait(barrier, plane - 1 + zs - 1)

    pending = []

    def send(src, dst, ssem, rsem, dev):
        return pltpu.make_async_remote_copy(
            src_ref=src, dst_ref=dst, send_sem=ssem, recv_sem=rsem, device_id=dev, device_id_type=MESH
        )

    def rs_copy(u, src, d):
        t = lax.rem(row + d, rows)
        return send(src.at[t], rsbuf.at[u, d - 1], rs_send.at[u, d - 1], rs_recv.at[u, d - 1], (t, col))

    def rs_copies(u, src):
        return [rs_copy(u, src, d) for d in range(1, rows)]

    def rs_start(u, src):
        for copy in rs_copies(u, src):
            copy.start()


    def rs_finish(u, src):
        total = src[row]
        for d, copy in enumerate(rs_copies(u, src)):
            copy.wait_recv()
            total = total + rsbuf[u, d]
        for copy in rs_copies(u, src):
            copy.wait_send()
        return total

    parts = up_send.shape[2]
    thick = width // parts

    def part_of(h):
        return pl.ds(h * thick, thick)

    def up_copy(u, s, h):
        ref = zbuf.at[u, s, part_of(h)]
        return send(ref, ref, up_send.at[u, s, h], up_recv.at[u, s, h], (row, col + 2))

    def dn_copy(u, s, h):
        ref = zbuf.at[u, s, part_of(h)]
        return send(ref, ref, dn_send.at[u, s, h], dn_recv.at[u, s, h], (row, col - 2))

    def slot_of(k, r):
        return k * rows + r

    def plane_copy(u, t, h, d):
        dst = rowbuf.at[u, slot_of(core, row), part_of(h)]
        return send(zbuf.at[u, t, part_of(h)], dst, pl_send.at[u, d, h], pl_recv.at[u, d, h], (t, col))

    def own_copy(u):
        return pltpu.make_async_copy(zbuf.at[u, row], rowbuf.at[u, slot_of(core, row)], own_sem.at[u])

    def to_plane(u, s, h):
        @pl.when(s != row)
        def _():
            plane_copy(u, s, h, lax.rem(s - row + rows, rows)).start()

        if h == parts - 1:
            @pl.when(s == row)
            def _():
                own_copy(u).start()

    def spread_put(u, piece):
        zbuf[u, z] = piece

    def spread_post(u, h):
        @pl.when(z + 1 < zs)
        def _():
            up_copy(u, z, h).start()

        @pl.when(z > 0)
        def _():
            dn_copy(u, z, h).start()

        to_plane(u, z, h)

    ahead = AHEAD

    def spread_step(u, s, h):
        low, high = z - s, z + s

        @pl.when(low >= 0)
        def _():
            up_copy(u, low, h).wait_recv()

            @pl.when(z + 1 < zs)
            def _():
                up_copy(u, low, h).start()

            to_plane(u, low, h)

        @pl.when(high < zs)
        def _():
            dn_copy(u, high, h).wait_recv()

            @pl.when(z > 0)
            def _():
                dn_copy(u, high, h).start()

            to_plane(u, high, h)

    waves = parts + LAG * (zs - 2)

    def spread_wave(u, w):
        for s in reversed(range(1, zs)):
            h = w - LAG * (s - 1)
            if 0 <= h < parts:
                spread_step(u, s, h)

    def spread_steps(u, fillers):
        waiting = list(fillers)
        for w in range(waves):
            while waiting and waiting[0][0] * waves <= w:
                waiting.pop(0)[1]()
            spread_wave(u, w)
            if w + ahead < parts:
                spread_post(u, w + ahead)
        for _, work_of in waiting:
            work_of()

    def partner_copy(u, d, h):
        ref = rowbuf.at[u, slot_of(core, lax.rem(row - d + rows, rows)), part_of(h)]
        return send(ref, ref, dd_send.at[u, d, h], dd_recv.at[u, d, h], (row, col + 1 - 2 * core))

    def spread_half(u):
        own_copy(u).wait()
        for h in range(parts):
            partner_copy(u, 0, h).start()
        for h in range(parts):
            for d in range(1, rows):
                plane_copy(u, row, h, d).wait_recv()
                partner_copy(u, d, h).start()

    def spread_rest(u):
        for h in range(parts):
            for d in range(rows):
                partner_copy(u, d, h).wait_recv()

    def spread_drain(u):
        for h in range(parts):
            for d in range(rows):
                partner_copy(u, d, h).wait_send()
            for d in range(1, rows):
                plane_copy(u, row, h, d).wait_send()
            for s in range(zs):
                @pl.when((z + 1 < zs) & (z >= s))
                def _():
                    up_copy(u, s, h).wait_send()

                @pl.when((z > 0) & (z <= s))
                def _():
                    dn_copy(u, s, h).wait_send()

    def ar_refs(u, m):
        deep = width * m // plane
        return deep, pl.ds(0, deep)

    def ar_one(u, m, d):
        deep, span = ar_refs(u, m)
        t = lax.rem(q + d, plane)
        return send(
            a_loc.at[u, t, span], a_in.at[u, d - 1, span], a_s1.at[u, d - 1], a_r1.at[u, d - 1], (t // 2, 2 * z + t % 2)
        )

    def ar_two(u, m, d):
        deep, span = ar_refs(u, m)
        t = lax.rem(z + d, zs)
        return send(
            a_z.at[u, z, span], a_z.at[u, z, span], a_s2.at[u, d - 1], a_r2.at[u, d - 1], (row, 2 * t + core)
        )

    def ar_three(u, m, d):
        deep, span = ar_refs(u, m)
        t = lax.rem(q + d, plane)
        return send(
            a_full.at[u, q, span], a_full.at[u, q, span], a_s3.at[u, d - 1], a_r3.at[u, d - 1],
            (t // 2, 2 * z + t % 2),
        )

    def ar_start(u, m, value):
        deep, span = ar_refs(u, m)
        for t in range(plane):
            a_loc[u, t, span] = value[t * deep : (t + 1) * deep]
        for d in range(1, plane):
            ar_one(u, m, d).start()

    def ar_mid(u, m):
        deep, span = ar_refs(u, m)
        total = a_loc[u, q, span]
        for d in range(1, plane):
            ar_one(u, m, d).wait_recv()
            total = total + a_in[u, d - 1, span]
        a_z[u, z, span] = total
        for d in range(1, zs):
            ar_two(u, m, d).start()

    def ar_late(u, m):
        deep, span = ar_refs(u, m)
        for d in range(1, zs):
            ar_two(u, m, d).wait_recv()
        total = a_z[u, 0, span]
        for s in range(1, zs):
            total = total + a_z[u, s, span]
        a_full[u, q, span] = total
        for d in range(1, plane):
            ar_three(u, m, d).start()

    def ar_finish(u, m):
        deep, span = ar_refs(u, m)
        for d in range(1, plane):
            ar_three(u, m, d).wait_recv()
        value = jnp.concatenate([a_full[u, t, span] for t in range(plane)], axis=0)
        for d in range(1, plane):
            ar_one(u, m, d).wait_send()
            ar_three(u, m, d).wait_send()
        for d in range(1, zs):
            ar_two(u, m, d).wait_send()
        return value

    def all_sum(u, m, value):
        ar_start(u, m, value)
        ar_mid(u, m)
        ar_late(u, m)
        return ar_finish(u, m)

    def load_covariance(begin, end):
        def chunk(i, carry):
            @pl.when(i + 1 < chunks)
            def _():
                fetch(i + 1).start()

            fetch(i).wait()

            def split(s, inner):
                for n in range(rows):
                    high, low = halves(stage[i % 2, pl.ds(s * 16, 16), n * wide : (n + 1) * wide])
                    ahi[n, pl.ds(i * deep + s * 16, 16), :] = high
                    alo[n, pl.ds(i * deep + s * 16, 16), :] = low
                return inner

            lax.fori_loop(0, deep // 16, split, 0, unroll=4)
            return carry

        lax.fori_loop(begin, end, chunk, 0)

    def half_span(k):
        return pl.ds(pl.multiple_of(k * (rows * wide), rows * wide), rows * wide)

    def split_half(u, k):
        def piece(i, carry):
            j = k * rows + i
            high, low = halves(rowbuf[u, j])
            wsplit[k, :width, pl.ds(pl.multiple_of(i * wide, wide), wide)] = high
            wsplit[k, width:, pl.ds(pl.multiple_of(i * wide, wide), wide)] = low
            return carry

        lax.fori_loop(0, rows, piece, 0)

    def half_term(k, n):
        go = functools.partial(lax.dot_general, dimension_numbers=NN, preferred_element_type=F32)
        one = go(wsplit[k], ahi[n, half_span(k), :])
        two = go(wsplit[k, :width], alo[n, half_span(k), :])
        return one[:width] + one[width:] + two

    early = min(EARLY, rows - 1)

    def product(u, rs):
        split_half(u, core)

        def near(d, carry):
            n = lax.rem(row + d, rows)
            part[n] = half_term(core, n)
            return carry

        lax.fori_loop(1, early + 1, near, 0)
        spread_rest(u)
        split_half(u, 1 - core)

        def far(d, carry):
            n = lax.rem(row + d, rows)
            part[n] = part[n] + half_term(1 - core, n)
            rs_copy(rs, part, d).start()
            return carry

        lax.fori_loop(1, early + 1, far, 0)

        def both(d, carry):
            n = lax.rem(row + d, rows)
            part[n] = half_term(core, n) + half_term(1 - core, n)

            @pl.when(d < rows)
            def _():
                rs_copy(rs, part, d).start()

            return carry

        lax.fori_loop(early + 1, rows + 1, both, 0)

    def scope(name):
        return jax.named_scope(name)

    def rows_to_basis(u, inverse, other, begin, end):
        def piece(j, carry):
            value = rowbuf[u, j]
            if other is not None:
                value = value - dot1(other, rowbuf[0, j], TN)
            value = dot3(inverse, value, NN)
            rowbuf[u, j] = value
            tall[u, pl.ds(pl.multiple_of(j * wide, wide), wide), :] = value.T * root
            return carry

        lax.fori_loop(begin, end, piece, 0)

    def tall_copy(u):
        return pltpu.make_async_copy(tall.at[u], tall_ref.at[u], out_sem.at[u])

    def first_copy(d, h):
        t = lax.rem(row + d, rows)
        return send(
            x_ref.at[t, part_of(h)], rsbuf.at[0, d - 1, part_of(h)], st_send.at[d - 1, h], st_recv.at[d - 1, h], (t, col)
        )

    def first_sum(h):
        span = part_of(h)
        total = x_ref[row, span]
        for d in range(1, rows):
            first_copy(d, h).wait_recv()
            total = total + rsbuf[0, d - 1, span]
        zbuf[0, z, span] = total
        spread_post(0, h)

    def multiply_and_sum(u):
        with scope(f"spread_half#{u}"):
            spread_half(u)
        with scope(f"product#{u}"):
            product(u, u + 1)

    with scope("start#0"):
        for h in range(parts):
            for d in range(1, rows):
                first_copy(d, h).start()
        done = chunks // 4
        load_covariance(0, done)
    with scope("spread_steps#0"):
        for h in range(parts):
            first_sum(h)
            more = chunks // 4 + (chunks - chunks // 4) * (h + 1) // (waves + 1)
            load_covariance(done, more)
            done = more
            if h > 0:
                spread_wave(0, h - 1)
        start = zbuf[0, z]
        ar_start(0, 1, dot(start, start, NT))
        for w in range(parts - 1, waves):
            more = chunks // 4 + (chunks - chunks // 4) * (w + 2) // (waves + 1)
            load_covariance(done, more)
            done = more
            spread_wave(0, w)
        for h in range(parts):
            for d in range(1, rows):
                first_copy(d, h).wait_send()
        ar_mid(0, 1)
    with scope("spread_half#0"):
        spread_half(0)
        ar_late(0, 1)
    with scope("product#0"):
        product(0, 1)
    with scope("factor#0"):
        gram = ar_finish(0, 1)
        upper0, inv0 = factor(gram, work)
        small_ref[0] = upper0
        small_ref[1] = inv0
        q0 = dot(inv0, start, NN)
        spread_drain(0)
    with scope("rs#1"):
        image = rs_finish(1, part)
    with scope("sum#1"):
        image0 = dot(inv0, image, NN)
        ar_start(1, 1, dot(q0, image0, NT))
        rows_to_basis(0, inv0, None, 0, cols // 2)
        ar_mid(1, 1)
        rows_to_basis(0, inv0, None, cols // 2, cols)
        ar_late(1, 1)
        tall_copy(0).start()
        h1 = ar_finish(1, 1)
        once = image0 - dot(h1, q0, TN)
    with scope("spread_start#1"):
        spread_put(1, once)
        for h in range(ahead):
            spread_post(1, h)
        ar_start(2, 2, jnp.concatenate([dot(q0, once, NT), dot(once, once, NT)], axis=0))

    panels = width // DEEP
    kept = {}

    def second_gram():
        both = ar_finish(2, 2)
        h2, raw = both[:width], both[width:]
        factor_begin(raw - dot(h2, h2, TN), work)
        small_ref[2] = h1
        small_ref[3] = h2
        kept["h2"] = h2

    def second_factor():
        h2 = kept["h2"]
        upper1, inv1 = factor_end(work)
        small_ref[4] = upper1
        small_ref[5] = inv1
        twice = once - dot(h2, q0, TN)
        kept["inv1"] = inv1
        kept["stacked"] = jnp.concatenate([q0, dot(inv1, twice, NN)], axis=0)
        kept["shift"] = dot(h2, image0, TN)

    with scope("spread_steps#1"):
        spread_steps(1, [
            (0.35, lambda: ar_mid(2, 2)), (0.7, lambda: ar_late(2, 2)),
        ])
    multiply_and_sum(1)
    with scope("factor#1"):
        second_gram()
        factor_panels(work, 0, panels)
        second_factor()
        spread_drain(1)
        h2, inv1, stacked = kept["h2"], kept["inv1"], kept["stacked"]
    with scope("rs#2"):
        image = rs_finish(2, part)
    with scope("last_start#0"):
        image1 = dot(inv1, image - kept["shift"], NN)
        spread_put(2, image1)
        spread_post(2, 0)
        ar_start(3, 2, dot(stacked, image1, NT))
        for h in range(1, ahead):
            spread_post(2, h)

    def basis_part(i):
        return lambda: rows_to_basis(1, inv1, h2, cols * i // 4, cols * (i + 1) // 4)

    def last_project():
        g1 = ar_finish(3, 2)
        once = image1 - dot(g1, stacked, TN)
        ar_start(4, 3, jnp.concatenate([dot(stacked, once, NT), dot(once, once, NT)], axis=0))
        small_ref[6] = g1[:width]
        small_ref[7] = g1[width:]
        kept["g1"] = g1

    def fold_spot(j, b):
        return pl.ds(pl.multiple_of(j * wide + b * width, width), width)

    def fold_part(i):
        def piece(j, carry):
            value = dot3(kept["g1"], jnp.concatenate([rowbuf[0, j], rowbuf[1, j]], axis=0), TN)
            for b in range(wide // width):
                tall[0, fold_spot(j, b), :] = value[:, b * width : (b + 1) * width]
            return carry

        return lambda: lax.fori_loop(cols * i // 4, cols * (i + 1) // 4, piece, 0)

    def fold():
        def piece(j, carry):
            for b in range(wide // width):
                span = slice(b * width, (b + 1) * width)
                rowbuf[2, j, :, span] = rowbuf[2, j, :, span] - tall[0, fold_spot(j, b), :]
            return carry

        lax.fori_loop(0, cols, piece, 0)

    def last_gram():
        both = ar_finish(4, 3)
        g2, raw = both[: 2 * width], both[2 * width :]
        small_ref[8] = g2[:width]
        small_ref[9] = g2[width:]
        factor_begin(raw - dot(g2, g2, TN), work)

    with scope("last_steps#0"):
        spread_steps(2, [
            (0.0, basis_part(0)),
            (0.1, lambda: ar_mid(3, 2)),
            (0.1, basis_part(1)),
            (0.25, lambda: ar_late(3, 2)),
            (0.25, basis_part(2)),
            (0.4, last_project),
            (0.41, basis_part(3)),
            (0.41, lambda: tall_copy(1).start()),
            (0.5, lambda: ar_mid(4, 3)),
            (0.5, lambda: tall_copy(0).wait()),
            (0.5, fold_part(0)),
            (0.6, fold_part(1)),
            (0.66, lambda: ar_late(4, 3)),
            (0.66, fold_part(2)),
            (0.8, fold_part(3)),
        ])
    with scope("last_gram#0"):
        last_gram()
        factor_panels(work, 0, panels // 2)
    with scope("last_half#0"):
        spread_half(2)
    with scope("factor#2"):
        factor_panels(work, panels // 2, panels)
        upper2, inv2 = factor_end(work)
        small_ref[10] = upper2
        small_ref[11] = inv2
    with scope("end#0"):
        spread_rest(2)
        spread_drain(2)
        fold()
        last = pltpu.make_async_copy(rowbuf.at[2], wide_ref, out_sem.at[2])
        last.start()
        tall_copy(1).wait()
        last.wait()


def main(rows, cols, x, covariance):
    row_count, col_count = covariance.shape
    width, wide = x.shape[1:]
    zs, plane = cols // 2, 2 * rows
    deep = min(256, row_count)
    dma = pltpu.SemaphoreType.DMA
    uses = 3
    sums, most = 5, 3 * width // plane
    return pl.pallas_call(
        functools.partial(main_kernel, rows, cols, float(rows * row_count) ** 0.5),
        out_shape=(
            jax.ShapeDtypeStruct((cols, width, wide), F32),
            jax.ShapeDtypeStruct((2, row_count, width), F32),
            jax.ShapeDtypeStruct((12, width, width), F32),
        ),
        in_specs=[pl.BlockSpec(memory_space=pltpu.VMEM), pl.BlockSpec(memory_space=pl.ANY)],
        out_specs=(pl.BlockSpec(memory_space=pl.ANY), pl.BlockSpec(memory_space=pl.ANY), pl.BlockSpec(memory_space=pltpu.VMEM)),
        scratch_shapes=[
            pltpu.VMEM((rows, row_count, wide), BF16),
            pltpu.VMEM((rows, row_count, wide), BF16),
            pltpu.VMEM((2, deep, col_count), F32),
            dma((2,)),
            pltpu.VMEM((rows, width, wide), F32),
            pltpu.VMEM((uses, rows - 1, width, wide), F32),
            dma((uses, rows - 1)), dma((uses, rows - 1)), dma((rows - 1, PARTS)), dma((rows - 1, PARTS)),
            pltpu.VMEM((uses, zs, width, wide), F32),
            dma((uses, zs, PARTS)), dma((uses, zs, PARTS)), dma((uses, zs, PARTS)), dma((uses, zs, PARTS)),
            pltpu.VMEM((uses, cols, width, wide), F32),
            dma((uses, rows, PARTS)), dma((uses, rows, PARTS)), dma((uses, rows, PARTS)), dma((uses, rows, PARTS)),
            dma((uses,)), dma((uses,)),
            pltpu.VMEM((sums, plane, most, width), F32),
            pltpu.VMEM((sums, plane - 1, most, width), F32),
            pltpu.VMEM((sums, zs, most, width), F32),
            pltpu.VMEM((sums, plane, most, width), F32),
            dma((sums, plane - 1)), dma((sums, plane - 1)),
            dma((sums, zs - 1)), dma((sums, zs - 1)),
            dma((sums, plane - 1)), dma((sums, plane - 1)),
            pltpu.VMEM((width, 2 * width), F32),
            pltpu.VMEM((2, 2 * width, rows * wide), BF16),
            pltpu.VMEM((2, row_count, width), F32),
        ],
        compiler_params=pltpu.CompilerParams(collective_id=0, has_side_effects=True, vmem_limit_bytes=LIMIT),
        name="lanczos",
    )(x, covariance)


def finish_kernel(root, wide_ref, tall_ref, small_ref, basis_ref, projection_ref, first_ref,
                  wide_buf, tall_buf, out_buf, wide_sem, tall_sem, out_sem):
    width = small_ref.shape[1]
    cols, _, wide = wide_buf.shape

    def get(j):
        rows_of = pl.ds(pl.multiple_of(j * wide, wide), wide)
        return (
            pltpu.make_async_copy(wide_ref.at[j], wide_buf.at[j], wide_sem.at[j]),
            pltpu.make_async_copy(tall_ref.at[:, rows_of], tall_buf.at[:, rows_of], tall_sem.at[j]),
            pltpu.make_async_copy(out_buf.at[rows_of], basis_ref.at[rows_of], out_sem.at[j]),
        )

    for j in range(cols):
        wide_in, tall_in, _ = get(j)
        wide_in.start()
        tall_in.start()
    upper0, inv0, h1, h2, upper1, inv1, g1a, g1b, g2a, g2b, upper2, inv2 = [small_ref[i] for i in range(12)]
    shift = jnp.concatenate([g2a, g2b], axis=0)

    def piece(j, carry):
        wide_in, tall_in, out = get(j)
        wide_in.wait()
        tall_in.wait()
        rows_of = pl.ds(pl.multiple_of(j * wide, wide), wide)
        q0, q1 = tall_buf[0, rows_of], tall_buf[1, rows_of]
        twice = wide_buf[j].T * root - dot1(jnp.concatenate([q0, q1], axis=1), shift, NN)
        out_buf[rows_of, :width] = q0
        out_buf[rows_of, width : 2 * width] = q1
        out_buf[rows_of, 2 * width :] = dot3(twice, inv2, NT)
        out.start()
        return carry

    lax.fori_loop(0, cols, piece, 0)
    zero = jnp.zeros((width, width), F32)
    spot = lambda i: pl.ds(i * width, width)
    for r, c, value in (
        (0, 0, h1 + h2), (1, 0, upper1), (2, 0, zero),
        (0, 1, g1a + g2a), (1, 1, g1b + g2b), (2, 1, upper2),
    ):
        projection_ref[spot(r), spot(c)] = value
    for r, c, value in ((0, 0, h1), (1, 0, zero), (2, 0, zero), (0, 1, g1a), (1, 1, g1b), (2, 1, zero)):
        first_ref[spot(r), spot(c)] = value
    lax.fori_loop(0, cols, lambda j, carry: (get(j)[2].wait(), carry)[1], 0)


def finish(order, wide_block, tall_blocks, small):
    cols, width, wide = wide_block.shape
    dma, vmem, anywhere = pltpu.SemaphoreType.DMA, pl.BlockSpec(memory_space=pltpu.VMEM), pl.BlockSpec(memory_space=pl.ANY)
    return pl.pallas_call(
        functools.partial(finish_kernel, float(order) ** 0.5),
        out_shape=(
            jax.ShapeDtypeStruct((cols * wide, 3 * width), F32),
            jax.ShapeDtypeStruct((3 * width, 2 * width), F32),
            jax.ShapeDtypeStruct((3 * width, 2 * width), F32),
        ),
        in_specs=[anywhere, anywhere, vmem],
        out_specs=(anywhere, vmem, vmem),
        scratch_shapes=[
            pltpu.VMEM(wide_block.shape, F32),
            pltpu.VMEM(tall_blocks.shape, F32),
            pltpu.VMEM((cols * wide, 3 * width), F32),
            dma((cols,)), dma((cols,)), dma((cols,)),
        ],
        compiler_params=pltpu.CompilerParams(vmem_limit_bytes=LIMIT),
        name="finish",
    )(wide_block, tall_blocks, small)


def solve(rows, cols, covariance, seed_index):
    x = gather(rows, covariance, seed_index)
    wide_block, tall_blocks, small = main(rows, cols, x, covariance)
    return finish(rows * covariance.shape[0], wide_block, tall_blocks, small)


def solution(mesh):
    rows, cols = mesh.shape["row"], mesh.shape["col"]
    return jax.shard_map(
        lambda covariance, seed_index: solve(rows, cols, covariance, seed_index),
        mesh=mesh,
        in_specs=(P("row", "col"), P()),
        out_specs=(P("row", None), P(), P()),
        check_vma=False,
    )
```
